32 devices in a mesh: dp: 4 (over x, core), fsdp: 4 (over z), mp: 2 (over y).
Axes of the slice: x: 2, y: 2, z: 4, core: 2. Of those that a mesh axis runs over, the one named last changes fastest.
Arguments:
- tokens_in: bfloat16 [4096, 3072], P(('dp', 'fsdp', 'mp')), may hold values from -40 to 40
- segment_ids: int32 [4096], P(('dp', 'fsdp', 'mp')), may hold values from 0 to 31, never falling along the last dimension, each value on 1 to 512 neighbouring positions
- target_ids: int32 [4096], P(('dp', 'fsdp', 'mp')), may hold values from 0 to 8191
- old_weights: bfloat16 [4, 3072, 2048], P(None, ('dp', 'fsdp', 'mp'))
- old_first: float32 [4, 3072, 2048], P(None, ('dp', 'fsdp', 'mp')), may hold values from -6 to 6
- old_second: float32 [4, 3072, 2048], P(None, ('dp', 'fsdp', 'mp')), may hold values from 0.01 to 4
- old_block: int32 [32], P(('dp', 'fsdp', 'mp')), may hold values from 0 to 31, each once
- new_residue: int32 [4], P('dp'), may hold values from 0 to 3, each once
- norm_gain: float32 [3072], replicated, may hold values from 0.5 to 1.5
- head_weight: bfloat16 [3072, 8192], P(None, ('fsdp', 'mp'))
Outputs:
- new_weights: bfloat16 [4, 3072, 2048], P(None, 'dp', ('fsdp', 'mp'))
- new_first: float32 [4, 3072, 2048], P(None, 'dp', ('fsdp', 'mp'))
- new_second: float32 [4, 3072, 2048], P(None, 'dp', ('fsdp', 'mp'))
- loss: float32 [4096], P(('dp', 'fsdp', 'mp'))
The draws below stay inside these ranges and needn't reach their ends.
Inputs may be any that keep to these rules, and one draw needn't show every extreme that they name: `old_block`: a permutation of the old layout's row blocks. `new_residue`: a permutation; index i of dp holds the rows whose number modulo 4 is new_residue[i], in rising order. `segment_ids`: never falling along the tokens.
All inputs are finite; a program needn't handle non-finite values.
Results may differ from the reference program's by a relative error of at most 0.0075.
Values may be sent and summed in bfloat16 or wider, within the bound.
A program may use at most 192 MiB of HBM per device.

```python
import math
import jax
import jax.numpy as jnp
import numpy as np
from jax import lax

D = 3072
HD = 128
HF = 2048
VOC = 8192
SEQ = 1024
TOKENS = 4096
N_DP = 4
N_FSDP = 4
N_MP = 2
DEVICES = 32


def draw_tokens_in(key, part):
    keys = jax.random.split(key, 1)
    drawn = jnp.clip(jax.random.normal(keys[0], (TOKENS, D), jnp.float32), -6.0, 6.0)
    return jnp.clip(drawn, -40.0, 40.0).astype(jnp.bfloat16)


def draw_old_weights(key, part):
    raw = jnp.clip(jax.random.normal(key, (4, D, HF), jnp.float32), -6.0, 6.0)
    fan_width = jnp.array([D, D, D, HF], jnp.float32).reshape(4, 1, 1)
    scaled = raw / jnp.sqrt(fan_width)
    return scaled.astype(jnp.bfloat16)


def draw_head_weight(key, part):
    keys = jax.random.split(key, 1)
    raw = jnp.clip(jax.random.normal(keys[0], (D, VOC), jnp.float32), -6.0, 6.0) / math.sqrt(D)
    return raw.astype(jnp.bfloat16)


def plant(result, own_key, least, largest):
    extent = result.shape
    index_at = [jax.random.randint(jax.random.fold_in(own_key, axis), (), 0, extent[axis]) for axis in range(len(extent))]
    result = result.at[tuple(index_at)].set(least)
    longest = extent.index(max(extent))
    index_at[longest] = (index_at[longest] + 1) % extent[longest]
    return result.at[tuple(index_at)].set(largest)


def levels(key, extent, cuts, low, top_value):
    def one(dim, shards_of):
        steps = jax.random.uniform(jax.random.fold_in(jax.random.fold_in(key, 6), dim), (shards_of,), jnp.float32, low / len(cuts), top_value / len(cuts))
        return jnp.repeat(jnp.exp(steps), extent[dim] // shards_of).reshape((-1,) + (1,) * (len(extent) - dim - 1))

    level = one(*cuts[0])
    for cut in cuts[1:]:
        level = level * one(*cut)
    return level


def rank_table(number_of, lean):
    loads = [(1 << 20) // math.isqrt(standing ** lean) + 1 for standing in range(1, number_of + 1)]
    deviation = 1 + sum(loads) // (1 << 30)
    return np.cumsum(np.array([max(1, weight // deviation) for weight in loads]))


def ranked(rng, dims, amount, slope):
    grid = rank_table(amount, slope)
    lot = jax.random.randint(jax.random.fold_in(rng, 1), dims, 0, int(grid[amount - 1]))
    grade = jnp.searchsorted(jnp.asarray(grid, jnp.int32), lot, side="right")
    return jax.random.permutation(jax.random.fold_in(rng, 2), amount)[grade].astype(jnp.int32)


def profile(number_of, total, bound, lean):
    loads = [(1 << 20) // math.isqrt(rank ** lean) + 1 for rank in range(2, number_of + 1)]
    spare, given = total - bound - (number_of - 1), [1] * (number_of - 1)
    while spare > 0:
        candidates = [i for i in range(number_of - 1) if given[i] < bound]
        pool, remaining = sum([loads[i] for i in candidates]), spare
        for i in candidates:
            addition = min(bound - given[i], max(1, remaining * loads[i] // pool), spare)
            given[i] = given[i] + addition
            spare = spare - addition
    return np.array([bound] + given)


def ragged(key, amount, total, reach, slope):
    if amount == 2:
        one = jax.random.randint(key, (), max(1, total - reach), min(reach, total - 1) + 1)
        return jnp.stack([one, total - one])
    lengths = jnp.asarray(profile(amount, total, reach, slope), jnp.int32)
    pairs = (amount - 1) // 2
    source_of, sink = lengths[1:1 + 2 * pairs:2], lengths[2:2 + 2 * pairs:2]
    margin = jnp.minimum(source_of - 1, reach - sink)
    moved = jax.random.randint(jax.random.fold_in(key, 1), (pairs,), 0, 1 << 20) % (margin + 1)
    lengths = lengths.at[1:1 + 2 * pairs:2].set(source_of - moved).at[2:2 + 2 * pairs:2].set(sink + moved)
    return lengths[jax.random.permutation(jax.random.fold_in(key, 2), amount)]


def centred(own_key, dims, spread, most, cuts=(), kind=jnp.bfloat16):
    values = jax.random.normal(own_key, dims, jnp.float32) * spread
    if len(cuts) > 0:
        values = levels(own_key, dims, cuts, -0.22, 0.18) * values
    return jnp.clip(values, min=-most, max=most).astype(kind)


def setup_inputs(seed: int = 0) -> dict:
    arg_keys = jax.random.split(jax.random.key(seed), 11)
    return {
        "tokens_in": draw_tokens_in(jax.random.fold_in(arg_keys[10], 71), 0),
        "segment_ids": jnp.searchsorted(jnp.cumsum(ragged(arg_keys[1], 8 * N_DP, TOKENS, SEQ // 2, 2)), jnp.arange(TOKENS), side="right").astype(jnp.int32),
        "target_ids": plant(ranked(arg_keys[2], (TOKENS,), VOC, 2), jax.random.fold_in(arg_keys[2], 3), 0, VOC - 1).astype(jnp.int32),
        "old_weights": draw_old_weights(jax.random.fold_in(arg_keys[10], 71), 0),
        "old_first": centred(arg_keys[4], (4, D, HF), 1.0, 6.0, ((1, 32),), jnp.float32),
        "old_second": jnp.clip(jnp.exp(math.log(4.0) - 5.9914646 * jax.random.uniform(arg_keys[5], (4, D, HF), jnp.float32) ** levels(arg_keys[5], (4, D, HF), ((1, 32),), -0.2, 0.2)), 0.01, 4.0),
        "old_block": jax.random.permutation(arg_keys[6], DEVICES).astype(jnp.int32),
        "new_residue": jax.random.permutation(arg_keys[7], N_DP).astype(jnp.int32),
        "norm_gain": jnp.clip(1.0 + 0.1 * jax.random.normal(arg_keys[8], (D,), jnp.float32), 0.5, 1.5),
        "head_weight": draw_head_weight(jax.random.fold_in(arg_keys[10], 71), 0),
    }


def inverse_table(table):
    total_count = table.shape[0]
    return jnp.zeros((total_count,), jnp.int32).at[table].set(jnp.arange(total_count, dtype=jnp.int32))

def logical_rows(stored, holder):
    matrices, row_count, columns = stored.shape
    devices = holder.shape[0]
    split_rows = stored.reshape(matrices, devices, row_count // devices, columns)
    return jnp.take(split_rows, holder, axis=1).reshape(matrices, row_count, columns)

def new_layout(logical, new_residue):
    matrices, row_count, columns = logical.shape
    dp_count = new_residue.shape[0]
    picked = jnp.take(logical.reshape(matrices, row_count // dp_count, dp_count, columns), new_residue, axis=2)
    return picked.transpose(0, 2, 1, 3).reshape(matrices, row_count, columns)

def one_sequence(tokens, segments, targets, weights, norm_gain, head_weight):
    seq_len = tokens.shape[0]
    columns = weights.shape[2]
    heads = columns // HD
    groups = N_FSDP * N_MP
    group_cols = columns // groups
    queries = jnp.dot(tokens, weights[0], preferred_element_type=jnp.float32).astype(jnp.bfloat16)
    keys_all = jnp.dot(tokens, weights[1], preferred_element_type=jnp.float32).astype(jnp.bfloat16)
    values_all = jnp.dot(tokens, weights[2], preferred_element_type=jnp.float32).astype(jnp.bfloat16)
    queries = queries.reshape(seq_len, heads, HD).astype(jnp.float32)
    keys_all = keys_all.reshape(seq_len, heads, HD).astype(jnp.float32)
    values_all = values_all.reshape(seq_len, heads, HD).astype(jnp.float32)
    positions = jnp.arange(seq_len, dtype=jnp.int32)
    allowed = (positions[:, None] >= positions[None, :]) & (segments[:, None] == segments[None, :])
    scores = jnp.einsum('shd,thd->hst', queries, keys_all) * (1.0 / math.sqrt(HD))
    scores = jnp.where(allowed[None], scores, -1e+30)
    row_max = lax.optimization_barrier(jnp.max(scores, axis=2, keepdims=True))
    expo = jnp.where(allowed[None], jnp.exp(scores - row_max), 0.0)
    soft = (expo / lax.optimization_barrier(jnp.sum(expo, axis=2, keepdims=True))).astype(jnp.bfloat16)
    attended = jnp.einsum('hst,thd->shd', soft.astype(jnp.float32), values_all).astype(jnp.bfloat16)
    attended = attended.reshape(seq_len, groups, group_cols).astype(jnp.float32)
    out_proj = weights[3].reshape(-1, groups, group_cols).astype(jnp.float32)
    parts = jnp.einsum('sgc,dgc->gsd', attended, out_proj).astype(jnp.bfloat16)
    parts = lax.optimization_barrier(parts)
    summed = lax.optimization_barrier(jnp.sum(parts.astype(jnp.float32), axis=0))
    hidden = tokens.astype(jnp.float32) + summed
    scale = lax.rsqrt(lax.optimization_barrier(jnp.mean(hidden * hidden, axis=1, keepdims=True)) + 1e-05)
    normed = (hidden * scale * norm_gain).astype(jnp.bfloat16)
    logits = jnp.dot(normed, head_weight, preferred_element_type=jnp.float32)
    row_top = lax.optimization_barrier(jnp.max(logits, axis=1))
    row_total = lax.optimization_barrier(jnp.sum(jnp.exp(logits - row_top[:, None]), axis=1))
    vocab_ids = jnp.arange(logits.shape[1], dtype=jnp.int32)
    picked = lax.optimization_barrier(jnp.sum(jnp.where(vocab_ids[None, :] == targets[:, None], logits, 0.0), axis=1))
    return row_top + jnp.log(row_total) - picked

def reference(tokens_in, segment_ids, target_ids, old_weights, old_first, old_second, old_block, new_residue, norm_gain, head_weight):
    holder = inverse_table(old_block)
    weights = logical_rows(old_weights, holder)
    new_weights = new_layout(weights, new_residue)
    new_first = new_layout(logical_rows(old_first, holder), new_residue)
    new_second = new_layout(logical_rows(old_second, holder), new_residue)
    seq_tokens = tokens_in.reshape(N_DP, SEQ, D)
    seq_segments = segment_ids.reshape(N_DP, SEQ)
    seq_targets = target_ids.reshape(N_DP, SEQ)

    def per_sequence(packed):
        return one_sequence(packed[0], packed[1], packed[2], weights, norm_gain, head_weight)
    losses = lax.map(per_sequence, (seq_tokens, seq_segments, seq_targets))
    return (new_weights, new_first, new_second, losses.reshape(TOKENS))
```

```python
import functools
import math

import jax
import jax.numpy as jnp
from jax import lax
from jax.experimental import pallas as pl
from jax.experimental.pallas import tpu as pltpu
from jax.sharding import PartitionSpec as P

HD = 128
LANES = 128
MESH = pl.DeviceIdType.MESH
ANY = pl.BlockSpec(memory_space=pl.ANY)
SMEM = pl.BlockSpec(memory_space=pltpu.SMEM)
VMEM = pl.BlockSpec(memory_space=pltpu.VMEM)
EVERYONE = ("dp", "fsdp", "mp")
VMEM_MOST = 60 * 1024 * 1024
CORES = 2


def inverse_of(table):
    total_count = table.shape[0]
    places = jnp.arange(total_count, dtype=jnp.int32)
    return jnp.sum(jnp.where(table[None, :] == places[:, None], places[None, :], 0), axis=1)


def share_tables(segment_ids, target_ids, old_block, new_residue):
    own = jnp.concatenate([segment_ids, target_ids, old_block, new_residue])
    rows = jnp.broadcast_to(own[None, None], (lax.axis_size(EVERYONE), 1, own.shape[0]))
    rows = lax.all_to_all(rows, EVERYONE, split_axis=0, concat_axis=0, tiled=True)[:, 0]
    count = segment_ids.shape[0]
    fm_count = lax.axis_size(("fsdp", "mp"))
    here = lax.dynamic_slice_in_dim(rows, lax.axis_index("dp") * fm_count, fm_count)
    segments = here[:, :count].reshape(-1)
    targets = here[:, count : 2 * count].reshape(-1)
    return segments, targets, rows[:, 2 * count], rows[::fm_count, 2 * count + 1]


def joint_loss(parts):
    axes = ("fsdp", "mp")
    fm_count = lax.axis_size(axes)
    own_count = parts.shape[1] // fm_count
    parts = parts.reshape(3, fm_count, own_count).transpose(1, 0, 2)
    parts = lax.all_to_all(parts, axes, split_axis=0, concat_axis=0, tiled=True)
    tops, totals, targets = parts[:, 0], parts[:, 1], parts[:, 2]
    joint_max = jnp.max(tops, axis=0)
    joint_total = jnp.sum(totals * jnp.exp(tops - joint_max[None]), axis=0)
    return joint_max + jnp.log(joint_total) - jnp.sum(targets, axis=0)


def pack_kernel(dp_count, fm_count, res_ref, old_ref, sent_ref, lanes):
    rows, columns = old_ref.shape[1:]
    pair_rows, group = rows // dp_count, columns // fm_count
    for c in range(columns // LANES):
        lanes[c] = old_ref[0, :, c * LANES : (c + 1) * LANES]
    for i in range(dp_count):
        for c in range(columns // LANES):
            f, at = divmod(c * LANES, group)
            chosen = lanes[c, pl.ds(res_ref[i], pair_rows, stride=dp_count), :]
            sent_ref[i * fm_count + f, 0, :, at : at + LANES] = chosen


def pack_moments(stored, residues, fm_count):
    matrices, row_count, columns = stored.shape
    dp_count = residues.shape[0]
    pair_rows, group = row_count // dp_count, columns // fm_count
    devices = dp_count * fm_count
    if pair_rows % 8:
        split_rows = stored.reshape(matrices, pair_rows, dp_count, fm_count, group)
        chosen = jnp.take(split_rows, residues, axis=2, mode="clip")
        return chosen.transpose(2, 3, 0, 1, 4).reshape(devices, matrices, pair_rows, group)
    return pl.pallas_call(
        functools.partial(pack_kernel, dp_count, fm_count),
        grid=(matrices,),
        out_shape=jax.ShapeDtypeStruct((devices, matrices, pair_rows, group), stored.dtype),
        in_specs=[SMEM, pl.BlockSpec((1, row_count, columns), lambda m: (m, 0, 0))],
        out_specs=pl.BlockSpec((devices, 1, pair_rows, group), lambda m: (0, m, 0, 0)),
        scratch_shapes=[pltpu.VMEM((columns // LANES, row_count, LANES), stored.dtype)],
        name="pack_moments",
    )(residues, stored)


def unpack_kernel(block_ref, got_ref, out_ref, buf, in_sems, out_sems):
    devices, _, pair_rows, _ = got_ref.shape
    for p in range(devices):
        pltpu.make_async_copy(got_ref.at[p], buf.at[p], in_sems.at[p]).start()
    for p in range(devices):
        pltpu.make_async_copy(got_ref.at[p], buf.at[p], in_sems.at[p]).wait()
        place = pl.ds(pl.multiple_of(block_ref[p] * pair_rows, pair_rows), pair_rows)
        pltpu.make_async_copy(buf.at[p], out_ref.at[:, place], out_sems.at[p]).start()
    for p in range(devices):
        place = pl.ds(pl.multiple_of(block_ref[p] * pair_rows, pair_rows), pair_rows)
        pltpu.make_async_copy(buf.at[p], out_ref.at[:, place], out_sems.at[p]).wait()


def unpack_moments(received, table, holder):
    devices, matrices, pair_rows, group = received.shape
    if pair_rows % 8:
        ordered = jnp.take(received, holder, axis=0, mode="clip")
        return ordered.transpose(1, 0, 2, 3).reshape(matrices, devices * pair_rows, group)
    return pl.pallas_call(
        unpack_kernel,
        out_shape=jax.ShapeDtypeStruct((matrices, devices * pair_rows, group), received.dtype),
        in_specs=[SMEM, ANY],
        out_specs=ANY,
        scratch_shapes=[
            pltpu.VMEM(received.shape, received.dtype),
            pltpu.SemaphoreType.DMA((devices,)),
            pltpu.SemaphoreType.DMA((devices,)),
        ],
        name="unpack_moments",
    )(table, received)


def remote(src, dst, send_sem, recv_sem, device):
    return pltpu.make_async_remote_copy(
        src_ref=src,
        dst_ref=dst,
        send_sem=send_sem,
        recv_sem=recv_sem,
        device_id=device,
        device_id_type=MESH,
    )


class Where:
    def __init__(self, sizes):
        self.n_dp, self.nf, self.nm = sizes
        self.nx, self.nfm = self.n_dp // CORES, self.nf * self.nm
        self.d, self.z, self.y = (lax.axis_index(name) for name in EVERYONE)
        self.x, self.c = self.d // CORES, self.d % CORES
        self.f = self.z * self.nm + self.y

    def fm_device(self, f):
        return (self.d, f // self.nm, f % self.nm)

    def greet(self):
        barrier = pltpu.get_barrier_semaphore()
        peers = [self.fm_device((self.f + j) % self.nfm) for j in range(1, self.nfm)]
        for k in range(1, self.nx):
            peers.append((((self.x + k) % self.nx) * CORES + self.c, self.z, self.y))
        peers.append((self.x * CORES + 1 - self.c, self.z, self.y))
        for peer in peers:
            pl.semaphore_signal(barrier, inc=1, device_id=peer, device_id_type=MESH)
        pl.semaphore_wait(barrier, len(peers))


class PlaneSpread:
    @staticmethod
    def sems(sizes):
        _, nf, nm = sizes
        dma = pltpu.SemaphoreType.DMA
        return [dma((nf,)), dma((nf,)), dma((nf,)), dma((nf, nm - 1)), dma((nf, nm - 1)), dma((1,))]

    def __init__(self, at, own, out, sems, base=0, arrived=None):
        self.at, self.own, self.out, self.base = at, own, out, base
        self.up, self.dn, self.ch, self.ys, self.yr, self.lc = sems
        self.arrived = arrived

    def slot(self, z, y):
        return self.out.at[self.base + z * self.at.nm + y]

    def _pass(self, zb, src, up, down):
        at = self.at
        dst = self.slot(zb, at.y)
        if up:
            pl.when(at.z + 1 < at.nf)(
                lambda: remote(src, dst, self.up.at[zb], self.ch.at[zb], (at.d, at.z + 1, at.y)).start()
            )
        if down:
            pl.when(at.z > 0)(
                lambda: remote(src, dst, self.dn.at[zb], self.ch.at[zb], (at.d, at.z - 1, at.y)).start()
            )
        for j in range(1, at.nm):
            there = (at.d, at.z, (at.y + j) % at.nm)
            remote(src, dst, self.ys.at[zb, j - 1], self.yr.at[zb, j - 1], there).start()
        if self.arrived:
            self.arrived(zb * at.nm + at.y, src)

    def begin(self):
        at = self.at
        self._pass(at.z, self.own, True, True)
        pltpu.make_async_copy(self.own, self.slot(at.z, at.y), self.lc.at[0]).start()

    def step(self, s):
        at = self.at

        def below():
            zb = at.z - s
            dst = self.slot(zb, at.y)
            remote(dst, dst, self.up.at[zb], self.ch.at[zb], (at.d, at.z, at.y)).wait_recv()
            self._pass(zb, dst, True, False)

        def above():
            zb = at.z + s
            dst = self.slot(zb, at.y)
            remote(dst, dst, self.dn.at[zb], self.ch.at[zb], (at.d, at.z, at.y)).wait_recv()
            self._pass(zb, dst, False, True)

        pl.when(at.z - s >= 0)(below)
        pl.when(at.z + s < at.nf)(above)

    def side(self, zb):
        at = self.at
        for j in range(1, at.nm):
            source = (at.y + at.nm - j) % at.nm
            dst = self.slot(zb, source)
            remote(dst, dst, self.ys.at[zb, j - 1], self.yr.at[zb, j - 1], (at.d, at.z, at.y)).wait_recv()
            if self.arrived:
                self.arrived(zb * at.nm + source, dst)

    def sides(self, s):
        at = self.at
        if s == 0:
            self.side(at.z)
        else:
            pl.when(at.z - s >= 0)(lambda: self.side(at.z - s))
            pl.when(at.z + s < at.nf)(lambda: self.side(at.z + s))

    def finish(self):
        at = self.at
        own = self.slot(at.z, at.y)
        pltpu.make_async_copy(self.own, own, self.lc.at[0]).wait()
        here = (at.d, at.z, at.y)
        for t in range(at.nf):
            for j in range(1, at.nm):
                remote(own, own, self.ys.at[t, j - 1], self.yr.at[t, j - 1], here).wait_send()
            pl.when((t <= at.z) & (at.z + 1 < at.nf))(
                lambda: remote(own, own, self.up.at[t], self.ch.at[t], here).wait_send()
            )
            pl.when((t >= at.z) & (at.z > 0))(
                lambda: remote(own, own, self.dn.at[t], self.ch.at[t], here).wait_send()
            )


class DpSpread:
    @staticmethod
    def sems(sizes):
        n_dp, nf, nm = sizes
        nfm, nx = nf * nm, n_dp // CORES
        dma = pltpu.SemaphoreType.DMA
        return [dma((nfm, max(nx - 1, 1))), dma((nfm, max(nx - 1, 1))), dma((nfm, nx)), dma((nfm, nx))]

    def __init__(self, at, out, sems):
        self.at, self.out = at, out
        self.xs, self.xr, self.cs, self.cr = sems

    def slot(self, x, c, f):
        return self.out.at[(x * CORES + c) * self.at.nfm + f]

    def send(self, f, src):
        at = self.at
        dst = self.slot(at.x, at.c, f)
        for k in range(1, at.nx):
            there = (((at.x + k) % at.nx) * CORES + at.c, at.z, at.y)
            remote(src, dst, self.xs.at[f, k - 1], self.xr.at[f, k - 1], there).start()
        there = (at.x * CORES + 1 - at.c, at.z, at.y)
        remote(src, dst, self.cs.at[f, 0], self.cr.at[f, 0], there).start()

    def forward(self, f):
        at = self.at
        here = (at.d, at.z, at.y)
        there = (at.x * CORES + 1 - at.c, at.z, at.y)
        for k in range(1, at.nx):
            dst = self.slot((at.x + at.nx - k) % at.nx, at.c, f)
            remote(dst, dst, self.xs.at[f, k - 1], self.xr.at[f, k - 1], here).wait_recv()
            remote(dst, dst, self.cs.at[f, k], self.cr.at[f, k], there).start()

    def finish(self):
        at = self.at
        here = (at.d, at.z, at.y)
        for f in range(at.nfm):
            for k in range(at.nx):
                dst = self.slot((at.x + at.nx - k) % at.nx, 1 - at.c, f)
                remote(dst, dst, self.cs.at[f, k], self.cr.at[f, k], here).wait_recv()
        for f in range(at.nfm):
            for k in range(at.nx):
                dst = self.slot(at.x, at.c, f)
                remote(dst, dst, self.cs.at[f, k], self.cr.at[f, k], here).wait_send()
            for k in range(1, at.nx):
                dst = self.slot(at.x, at.c, f)
                remote(dst, dst, self.xs.at[f, k - 1], self.xr.at[f, k - 1], here).wait_send()


def inputs_kernel(sizes, tok_ref, w_ref, xall_ref, wall_ref, as_sem, ar_sem, wl_sem, *sems):
    at = Where(sizes)
    group = wall_ref.shape[3]
    plane = PlaneSpread(at, tok_ref, xall_ref, sems[:6])
    along = DpSpread(at, wall_ref, sems[6:10])
    at.greet()
    mine = wall_ref.at[at.d * at.nfm + at.f]

    def columns(f):
        return w_ref.at[0:3, :, pl.ds(pl.multiple_of(f * group, group), group)]

    for j in range(1, at.nfm):
        f = (at.f + j) % at.nfm
        remote(columns(f), mine, as_sem.at[j - 1], ar_sem.at[j - 1], at.fm_device(f)).start()
    plane.begin()
    local = pltpu.make_async_copy(columns(at.f), mine, wl_sem.at[0])
    local.start()
    along.send(at.f, columns(at.f))
    for j in range(1, at.nfm):
        f = (at.f + at.nfm - j) % at.nfm
        dst = wall_ref.at[at.d * at.nfm + f]
        remote(dst, dst, as_sem.at[j - 1], ar_sem.at[j - 1], at.fm_device(f)).wait_recv()
        along.send(f, dst)
    for s in range(1, at.nf):
        plane.step(s)
        if s == 1:
            for j in range(at.nfm):
                along.forward((at.f + at.nfm - j) % at.nfm)
    for s in range(at.nf):
        plane.sides(s)
    along.finish()
    plane.finish()
    local.wait()
    for j in range(1, at.nfm):
        remote(mine, mine, as_sem.at[j - 1], ar_sem.at[j - 1], at.fm_device(at.f)).wait_send()


def share_inputs(sizes, tokens_in, old_weights):
    n_dp, nf, nm = sizes
    nfm = nf * nm
    rows, columns = old_weights.shape[1:]
    dma = pltpu.SemaphoreType.DMA
    return pl.pallas_call(
        functools.partial(inputs_kernel, sizes),
        out_shape=(
            jax.ShapeDtypeStruct((nfm,) + tokens_in.shape, tokens_in.dtype),
            jax.ShapeDtypeStruct((n_dp * nfm, 3, rows, columns // nfm), old_weights.dtype),
        ),
        in_specs=[ANY, ANY],
        out_specs=(ANY, ANY),
        scratch_shapes=[dma((nfm - 1,)), dma((nfm - 1,)), dma((1,))]
        + PlaneSpread.sems(sizes)
        + DpSpread.sems(sizes),
        compiler_params=pltpu.CompilerParams(collective_id=0, has_side_effects=True),
        name="share_inputs",
    )(tokens_in, old_weights)


def outputs_kernel(sizes, att_ref, w_ref, aall_ref, oall_ref, *sems):
    at = Where(sizes)
    plane = PlaneSpread(at, att_ref, aall_ref, sems[:6])
    along = DpSpread(at, oall_ref, sems[12:16])
    wide = PlaneSpread(at, w_ref.at[3], oall_ref, sems[6:12], at.d * at.nfm, along.send)
    at.greet()
    plane.begin()
    wide.begin()
    for s in range(1, at.nf):
        plane.step(s)
        wide.step(s)
    for s in range(at.nf):
        plane.sides(s)
        wide.sides(s)
    for f in range(at.nfm):
        along.forward((at.f + f) % at.nfm)
    along.finish()
    plane.finish()
    wide.finish()


def share_outputs(sizes, attended, old_weights):
    n_dp, nf, nm = sizes
    nfm = nf * nm
    rows, columns = old_weights.shape[1:]
    return pl.pallas_call(
        functools.partial(outputs_kernel, sizes),
        out_shape=(
            jax.ShapeDtypeStruct((nfm,) + attended.shape, attended.dtype),
            jax.ShapeDtypeStruct((n_dp * nfm, rows, columns), old_weights.dtype),
        ),
        in_specs=[ANY, ANY],
        out_specs=(ANY, ANY),
        scratch_shapes=PlaneSpread.sems(sizes) + PlaneSpread.sems(sizes) + DpSpread.sems(sizes),
        compiler_params=pltpu.CompilerParams(collective_id=1, has_side_effects=True),
        name="share_outputs",
    )(attended, old_weights)


def keep_residue(full, wide_ref, chosen_ref, res, dp_count):
    rows = wide_ref.shape[1] // dp_count
    for c in range(wide_ref.shape[0]):
        at = slice(c * LANES, (c + 1) * LANES)
        wide_ref[c] = full[:, at].astype(jnp.float32)
        chosen_ref[:, at] = wide_ref[c, pl.ds(res, rows, stride=dp_count), :].astype(chosen_ref.dtype)


def attend_kernel(
    dp_count, place_ref, res_ref, x_ref, wall_ref, segr_ref, segc_ref, att_ref, kept_ref, wbuf, wide, q_ref, k_ref, v_ref, sems
):
    blocks, _, rows, _ = wall_ref.shape
    seq, group = att_ref.shape

    def fetch(p):
        at = pl.ds(pl.multiple_of(place_ref[p] * rows, rows), rows)
        return pltpu.make_async_copy(wall_ref.at[p], wbuf.at[:, at], sems.at[p])

    for p in range(blocks):
        fetch(p).start()
    for p in range(blocks):
        fetch(p).wait()
    tile = 256

    def project(i, carry):
        at = pl.ds(pl.multiple_of(i * tile, tile), tile)
        x = x_ref[at, :]
        for m, ref in enumerate((q_ref, k_ref, v_ref)):
            ref[at, :] = jnp.dot(x, wbuf[m], preferred_element_type=jnp.float32).astype(jnp.bfloat16)
        return carry

    lax.fori_loop(0, seq // tile, project, 0)
    scale = 1.0 / math.sqrt(HD)
    for i in range(seq // tile):
        low, high = i * tile, (i + 1) * tile
        rowid = lax.broadcasted_iota(jnp.int32, (tile, high), 0) + low
        colid = lax.broadcasted_iota(jnp.int32, (tile, high), 1)
        allowed = (rowid >= colid) & (segc_ref[low:high, :1] == segr_ref[:1, :high])
        for h in range(group // HD):
            cols = slice(h * HD, (h + 1) * HD)
            scores = lax.dot_general(
                q_ref[low:high, cols], k_ref[:high, cols], (((1,), (1,)), ((), ())), preferred_element_type=jnp.float32
            )
            scores = jnp.where(allowed, scores * scale, -1e30)
            expo = jnp.exp(scores - jnp.max(scores, axis=1, keepdims=True))
            soft = (expo / jnp.sum(expo, axis=1, keepdims=True)).astype(jnp.bfloat16)
            out = jnp.dot(soft, v_ref[:high, cols], preferred_element_type=jnp.float32)
            att_ref[low:high, cols] = out.astype(jnp.bfloat16)
    for m in range(3):
        keep_residue(wbuf.at[m], wide, kept_ref.at[m], res_ref[0], dp_count)


def attend(dp_count, place, own_res, x_full, wall, segments):
    seq, width = x_full.shape
    blocks, _, rows, group = wall.shape
    bf16, f32 = jnp.bfloat16, jnp.float32
    return pl.pallas_call(
        functools.partial(attend_kernel, dp_count),
        out_shape=(
            jax.ShapeDtypeStruct((seq, group), bf16),
            jax.ShapeDtypeStruct((3, width // dp_count, group), bf16),
        ),
        in_specs=[SMEM, SMEM, VMEM, ANY, VMEM, VMEM],
        out_specs=(VMEM, VMEM),
        scratch_shapes=[
            pltpu.VMEM((3, width, group), bf16),
            pltpu.VMEM((group // LANES, width, LANES), f32),
            pltpu.VMEM((seq, group), bf16),
            pltpu.VMEM((seq, group), bf16),
            pltpu.VMEM((seq, group), bf16),
            pltpu.SemaphoreType.DMA((blocks,)),
        ],
        compiler_params=pltpu.CompilerParams(vmem_limit_bytes=VMEM_MOST),
        cost_estimate=pl.CostEstimate(flops=8 * 10**9, bytes_accessed=3 * 10**7, transcendentals=10**6),
        name="attend",
    )(place, own_res, x_full, wall, segments[None, :], segments[:, None])


def head_kernel(
    dp_count, place_ref, res_ref, f_ref, x_ref, a_ref, oall_ref, hw_ref, gain_ref, tgt_ref, out_ref, kept_ref,
    obuf, hbuf, wide, abuf, hid, norm, sems, hsem,
):
    blocks, rows, columns = oall_ref.shape
    tile, width = x_ref.shape
    fm_count, _, group = a_ref.shape
    vocab = hw_ref.shape[1]
    chunk = 256

    def fetch(p):
        at = pl.ds(pl.multiple_of(place_ref[p] * rows, rows), rows)
        return pltpu.make_async_copy(oall_ref.at[p], obuf.at[at], sems.at[p])

    def fetch_head():
        return pltpu.make_async_copy(hw_ref, hbuf, hsem.at[0])

    @pl.when(pl.program_id(0) == 0)
    def _():
        for p in range(blocks):
            fetch(p).start()
        fetch_head().start()
        for p in range(blocks):
            fetch(p).wait()

    for f in range(fm_count):
        abuf[:, f * group : (f + 1) * group] = a_ref[f]

    def hidden(i, total):
        at = pl.ds(pl.multiple_of(i * chunk, chunk), chunk)
        part = lax.dot_general(
            abuf[...], obuf[at, :], (((1,), (1,)), ((), ())), preferred_element_type=jnp.float32
        )
        part = part + x_ref[:, at].astype(jnp.float32)
        hid[:, at] = part
        return total + jnp.sum(part * part, axis=1, keepdims=True)

    total = lax.fori_loop(0, width // chunk, hidden, jnp.zeros((tile, 1), jnp.float32))
    scale = lax.rsqrt(total / width + 1e-05)

    def normed(i, carry):
        at = pl.ds(pl.multiple_of(i * chunk, chunk), chunk)
        norm[:, at] = (hid[:, at] * scale * gain_ref[:, at]).astype(jnp.bfloat16)
        return carry

    lax.fori_loop(0, width // chunk, normed, 0)

    @pl.when(pl.program_id(0) == 0)
    def _():
        fetch_head().wait()
        own = pl.ds(pl.multiple_of(f_ref[0] * group, group), group)
        keep_residue(obuf[:, own], wide, kept_ref, res_ref[0], dp_count)

    local = tgt_ref[:, :1] - f_ref[0] * vocab
    lane = lax.broadcasted_iota(jnp.int32, (tile, chunk), 1)

    def score(i, carry):
        top, total, picked = carry
        at = pl.ds(pl.multiple_of(i * chunk, chunk), chunk)
        logits = jnp.dot(norm[...], hbuf[:, at], preferred_element_type=jnp.float32)
        higher = jnp.maximum(top, jnp.max(logits, axis=1, keepdims=True))
        total = total * jnp.exp(top - higher) + jnp.sum(jnp.exp(logits - higher), axis=1, keepdims=True)
        hit = jnp.where(lane + i * chunk == local, logits, 0.0)
        return higher, total, picked + jnp.sum(hit, axis=1, keepdims=True)

    zero = jnp.zeros((tile, 1), jnp.float32)
    top, total, picked = lax.fori_loop(0, vocab // chunk, score, (zero - 1e30, zero, zero))
    lanes = lax.broadcasted_iota(jnp.int32, (tile, 128), 1)
    out_ref[...] = jnp.where(lanes == 0, top, jnp.where(lanes == 1, total, picked))


def head_parts(dp_count, place, own_res, own_f, x_full, a_all, oall, head_weight, norm_gain, targets):
    seq, width = x_full.shape
    fm_count, _, group = a_all.shape
    blocks, rows, columns = oall.shape
    vocab = head_weight.shape[1]
    tile = 256
    bf16, f32 = jnp.bfloat16, jnp.float32
    return pl.pallas_call(
        functools.partial(head_kernel, dp_count),
        grid=(seq // tile,),
        out_shape=(
            jax.ShapeDtypeStruct((seq, 128), f32),
            jax.ShapeDtypeStruct((width // dp_count, group), bf16),
        ),
        in_specs=[
            SMEM,
            SMEM,
            SMEM,
            pl.BlockSpec((tile, width), lambda i: (i, 0)),
            pl.BlockSpec((fm_count, tile, group), lambda i: (0, i, 0)),
            ANY,
            ANY,
            pl.BlockSpec((1, width), lambda i: (0, 0)),
            pl.BlockSpec((tile, 1), lambda i: (i, 0)),
        ],
        out_specs=(
            pl.BlockSpec((tile, 128), lambda i: (i, 0)),
            pl.BlockSpec((width // dp_count, group), lambda i: (0, 0)),
        ),
        scratch_shapes=[
            pltpu.VMEM((width, columns), bf16),
            pltpu.VMEM((width, vocab), bf16),
            pltpu.VMEM((group // LANES, width, LANES), f32),
            pltpu.VMEM((tile, columns), bf16),
            pltpu.VMEM((tile, width), f32),
            pltpu.VMEM((tile, width), bf16),
            pltpu.SemaphoreType.DMA((blocks,)),
            pltpu.SemaphoreType.DMA((1,)),
        ],
        compiler_params=pltpu.CompilerParams(vmem_limit_bytes=VMEM_MOST),
        cost_estimate=pl.CostEstimate(flops=2 * 10**10, bytes_accessed=4 * 10**7, transcendentals=10**6),
        name="head_parts",
    )(place, own_res, own_f, x_full, a_all, oall, head_weight, norm_gain[None, :], targets[:, None])


def in_blocks(wall, table, holder):
    if wall.shape[-2] % 16 == 0:
        return wall, table
    ordered = jnp.take(wall, holder, axis=0, mode="clip")
    blocks, rows = ordered.shape[0], ordered.shape[-2]
    join = 16 // math.gcd(16, rows)
    middle = ordered.shape[1:-2]
    ordered = ordered.reshape((blocks // join, join) + middle + ordered.shape[-2:])
    ordered = jnp.moveaxis(ordered, 1, -3)
    ordered = ordered.reshape((blocks // join,) + middle + (join * rows, ordered.shape[-1]))
    return ordered, jnp.arange(blocks // join, dtype=jnp.int32)


def body(
    sizes,
    tokens_in,
    segment_ids,
    target_ids,
    old_weights,
    old_first,
    old_second,
    old_block,
    new_residue,
    norm_gain,
    head_weight,
):
    dp_count, nf, nm = sizes
    fm_count = nf * nm
    segments, targets, table, residues = share_tables(segment_ids, target_ids, old_block, new_residue)
    holder = inverse_of(table)
    own_f = lax.axis_index(("fsdp", "mp"))[None]
    first_sent = pack_moments(old_first, residues, fm_count)
    second_sent = pack_moments(old_second, residues, fm_count)
    first_got = lax.all_to_all(first_sent, EVERYONE, split_axis=0, concat_axis=0, tiled=True)
    second_got = lax.all_to_all(second_sent, EVERYONE, split_axis=0, concat_axis=0, tiled=True)
    x_all, wall = share_inputs(sizes, tokens_in, old_weights)
    x_full = x_all.reshape(-1, tokens_in.shape[1])
    wall, place = in_blocks(wall, table, holder)
    attended, kept = attend(dp_count, place, new_residue, x_full, wall, segments)
    a_all, oall = share_outputs(sizes, attended, old_weights)
    oall, place = in_blocks(oall, table, holder)
    parts, kept_out = head_parts(
        dp_count, place, new_residue, own_f, x_full, a_all, oall, head_weight, norm_gain, targets
    )
    loss = joint_loss(parts[:, :3].T)
    new_weights = jnp.concatenate([kept, kept_out[None]])
    new_first = unpack_moments(first_got, table, holder)
    new_second = unpack_moments(second_got, table, holder)
    return (new_weights, new_first, new_second, loss)


def solution(mesh):
    placed = (
        P(EVERYONE, None),
        P(EVERYONE),
        P(EVERYONE),
        P(None, EVERYONE, None),
        P(None, EVERYONE, None),
        P(None, EVERYONE, None),
        P(EVERYONE),
        P("dp"),
        P(),
        P(None, ("fsdp", "mp")),
    )
    sizes = tuple(mesh.shape[name] for name in EVERYONE)
    return jax.shard_map(
        functools.partial(body, sizes),
        mesh=mesh,
        in_specs=placed,
        out_specs=(
            P(None, "dp", ("fsdp", "mp")),
            P(None, "dp", ("fsdp", "mp")),
            P(None, "dp", ("fsdp", "mp")),
            P(EVERYONE),
        ),
        check_vma=False,
    )
```

```python
import functools
import math

import jax
import jax.numpy as jnp
from jax import lax
from jax.experimental import pallas as pl
from jax.experimental.pallas import tpu as pltpu
from jax.sharding import PartitionSpec as P

HD = 128
LANES = 128
MESH = pl.DeviceIdType.MESH
ANY = pl.BlockSpec(memory_space=pl.ANY)
SMEM = pl.BlockSpec(memory_space=pltpu.SMEM)
VMEM = pl.BlockSpec(memory_space=pltpu.VMEM)
EVERYONE = ("dp", "fsdp", "mp")
VMEM_MOST = 60 * 1024 * 1024
CORES = 2
EARLY = 3
EARLY_STEP = 1
ROW_TILE = 256


def inverse_of(table):
    total_count = table.shape[0]
    places = jnp.arange(total_count, dtype=jnp.int32)
    return jnp.sum(jnp.where(table[None, :] == places[:, None], places[None, :], 0), axis=1)


def share_tables(segment_ids, target_ids, old_block, new_residue):
    own = jnp.concatenate([segment_ids, target_ids, old_block, new_residue])
    rows = jnp.broadcast_to(own[None, None], (lax.axis_size(EVERYONE), 1, own.shape[0]))
    rows = lax.all_to_all(rows, EVERYONE, split_axis=0, concat_axis=0, tiled=True)[:, 0]
    count = segment_ids.shape[0]
    fm_count = lax.axis_size(("fsdp", "mp"))
    here = lax.dynamic_slice_in_dim(rows, lax.axis_index("dp") * fm_count, fm_count)
    segments = here[:, :count].reshape(-1)
    targets = here[:, count : 2 * count].reshape(-1)
    return segments, targets, rows[:, 2 * count], rows[::fm_count, 2 * count + 1]


def joint_loss(parts):
    axes = ("fsdp", "mp")
    fm_count = lax.axis_size(axes)
    own_count = parts.shape[1] // fm_count
    parts = parts.reshape(3, fm_count, own_count).transpose(1, 0, 2)
    parts = lax.all_to_all(parts, axes, split_axis=0, concat_axis=0, tiled=True)
    tops, totals, targets = parts[:, 0], parts[:, 1], parts[:, 2]
    joint_max = jnp.max(tops, axis=0)
    joint_total = jnp.sum(totals * jnp.exp(tops - joint_max[None]), axis=0)
    return joint_max + jnp.log(joint_total) - jnp.sum(targets, axis=0)


def pack_kernel(dp_count, fm_count, res_ref, old_ref, sent_ref, lanes):
    rows, columns = old_ref.shape[1:]
    pair_rows, group = rows // dp_count, columns // fm_count
    for c in range(columns // LANES):
        lanes[c] = old_ref[0, :, c * LANES : (c + 1) * LANES]
    for i in range(dp_count):
        for c in range(columns // LANES):
            f, at = divmod(c * LANES, group)
            chosen = lanes[c, pl.ds(res_ref[i], pair_rows, stride=dp_count), :]
            sent_ref[i * fm_count + f, 0, :, at : at + LANES] = chosen


def pack_moments(stored, residues, fm_count):
    matrices, row_count, columns = stored.shape
    dp_count = residues.shape[0]
    pair_rows, group = row_count // dp_count, columns // fm_count
    devices = dp_count * fm_count
    if pair_rows % 8:
        split_rows = stored.reshape(matrices, pair_rows, dp_count, fm_count, group)
        chosen = jnp.take(split_rows, residues, axis=2, mode="clip")
        return chosen.transpose(2, 3, 0, 1, 4).reshape(devices, matrices, pair_rows, group)
    return pl.pallas_call(
        functools.partial(pack_kernel, dp_count, fm_count),
        grid=(matrices,),
        out_shape=jax.ShapeDtypeStruct((devices, matrices, pair_rows, group), stored.dtype),
        in_specs=[SMEM, pl.BlockSpec((1, row_count, columns), lambda m: (m, 0, 0))],
        out_specs=pl.BlockSpec((devices, 1, pair_rows, group), lambda m: (0, m, 0, 0)),
        scratch_shapes=[pltpu.VMEM((columns // LANES, row_count, LANES), stored.dtype)],
        name="pack_moments",
    )(residues, stored)


def unpack_kernel(which, block_ref, got_ref, out_ref, buf, in_sems, out_sems):
    if which is not None:
        got_ref = got_ref.at[which]
    devices, _, pair_rows, _ = got_ref.shape
    for p in range(devices):
        pltpu.make_async_copy(got_ref.at[p], buf.at[p], in_sems.at[p]).start()
    for p in range(devices):
        pltpu.make_async_copy(got_ref.at[p], buf.at[p], in_sems.at[p]).wait()
        place = pl.ds(pl.multiple_of(block_ref[p] * pair_rows, pair_rows), pair_rows)
        pltpu.make_async_copy(buf.at[p], out_ref.at[:, place], out_sems.at[p]).start()
    for p in range(devices):
        place = pl.ds(pl.multiple_of(block_ref[p] * pair_rows, pair_rows), pair_rows)
        pltpu.make_async_copy(buf.at[p], out_ref.at[:, place], out_sems.at[p]).wait()


def unpack_moments(received, table, holder, which=None):
    devices, matrices, pair_rows, group = received.shape[-4:]
    if pair_rows % 8:
        ordered = jnp.take(received, holder, axis=0, mode="clip")
        return ordered.transpose(1, 0, 2, 3).reshape(matrices, devices * pair_rows, group)
    return pl.pallas_call(
        functools.partial(unpack_kernel, which),
        out_shape=jax.ShapeDtypeStruct((matrices, devices * pair_rows, group), received.dtype),
        in_specs=[SMEM, ANY],
        out_specs=ANY,
        scratch_shapes=[
            pltpu.VMEM(received.shape[-4:], received.dtype),
            pltpu.SemaphoreType.DMA((devices,)),
            pltpu.SemaphoreType.DMA((devices,)),
        ],
        name="unpack_moments",
    )(table, received)


def remote(src, dst, send_sem, recv_sem, device):
    return pltpu.make_async_remote_copy(
        src_ref=src,
        dst_ref=dst,
        send_sem=send_sem,
        recv_sem=recv_sem,
        device_id=device,
        device_id_type=MESH,
    )


class Where:
    def __init__(self, sizes):
        self.n_dp, self.nf, self.nm = sizes
        self.nx, self.nfm = self.n_dp // CORES, self.nf * self.nm
        self.d, self.z, self.y = (lax.axis_index(name) for name in EVERYONE)
        self.x, self.c = self.d // CORES, self.d % CORES
        self.f = self.z * self.nm + self.y

    def fm_device(self, f):
        return (self.d, f // self.nm, f % self.nm)

    def greet(self, diagonal=False):
        barrier = pltpu.get_barrier_semaphore()
        peers = [self.fm_device((self.f + j) % self.nfm) for j in range(1, self.nfm)]
        for k in range(1, self.nx):
            peers.append((((self.x + k) % self.nx) * CORES + self.c, self.z, self.y))
            if diagonal:
                peers.append((((self.x + k) % self.nx) * CORES + 1 - self.c, self.z, self.y))
        peers.append((self.x * CORES + 1 - self.c, self.z, self.y))
        for peer in peers:
            pl.semaphore_signal(barrier, inc=1, device_id=peer, device_id_type=MESH)
        pl.semaphore_wait(barrier, len(peers))


class PlaneSpread:
    @staticmethod
    def sems(sizes):
        _, nf, nm = sizes
        dma = pltpu.SemaphoreType.DMA
        return [dma((nf,)), dma((nf,)), dma((nf,)), dma((nf, nm - 1)), dma((nf, nm - 1)), dma((1,))]

    def __init__(self, at, own, out, sems, base=0, arrived=None, rows=None):
        self.at, self.own, self.out, self.base, self.rows = at, own, out, base, rows
        self.up, self.dn, self.ch, self.ys, self.yr, self.lc = sems
        self.arrived = arrived

    def slot(self, z, y):
        slot = self.base + z * self.at.nm + y
        return self.out.at[slot] if self.rows is None else self.out.at[slot, self.rows]

    def _pass(self, zb, src, up, down):
        at = self.at
        dst = self.slot(zb, at.y)
        if up:
            pl.when(at.z + 1 < at.nf)(
                lambda: remote(src, dst, self.up.at[zb], self.ch.at[zb], (at.d, at.z + 1, at.y)).start()
            )
        if down:
            pl.when(at.z > 0)(
                lambda: remote(src, dst, self.dn.at[zb], self.ch.at[zb], (at.d, at.z - 1, at.y)).start()
            )
        for j in range(1, at.nm):
            there = (at.d, at.z, (at.y + j) % at.nm)
            remote(src, dst, self.ys.at[zb, j - 1], self.yr.at[zb, j - 1], there).start()
        if self.arrived:
            self.arrived(zb * at.nm + at.y, src)

    def begin(self):
        at = self.at
        self._pass(at.z, self.own, True, True)
        pltpu.make_async_copy(self.own, self.slot(at.z, at.y), self.lc.at[0]).start()

    def step(self, s):
        at = self.at

        def below():
            zb = at.z - s
            dst = self.slot(zb, at.y)
            remote(dst, dst, self.up.at[zb], self.ch.at[zb], (at.d, at.z, at.y)).wait_recv()
            self._pass(zb, dst, True, False)

        def above():
            zb = at.z + s
            dst = self.slot(zb, at.y)
            remote(dst, dst, self.dn.at[zb], self.ch.at[zb], (at.d, at.z, at.y)).wait_recv()
            self._pass(zb, dst, False, True)

        pl.when(at.z - s >= 0)(below)
        pl.when(at.z + s < at.nf)(above)

    def side(self, zb):
        at = self.at
        for j in range(1, at.nm):
            source = (at.y + at.nm - j) % at.nm
            dst = self.slot(zb, source)
            remote(dst, dst, self.ys.at[zb, j - 1], self.yr.at[zb, j - 1], (at.d, at.z, at.y)).wait_recv()
            if self.arrived:
                self.arrived(zb * at.nm + source, dst)

    def sides(self, s):
        at = self.at
        if s == 0:
            self.side(at.z)
        else:
            pl.when(at.z - s >= 0)(lambda: self.side(at.z - s))
            pl.when(at.z + s < at.nf)(lambda: self.side(at.z + s))

    def finish(self):
        own = self.slot(self.at.z, self.at.y)
        pltpu.make_async_copy(self.own, own, self.lc.at[0]).wait()
        self.sent()

    def sent(self):
        at = self.at
        own = self.slot(at.z, at.y)
        here = (at.d, at.z, at.y)
        for t in range(at.nf):
            for j in range(1, at.nm):
                remote(own, own, self.ys.at[t, j - 1], self.yr.at[t, j - 1], here).wait_send()
            pl.when((t <= at.z) & (at.z + 1 < at.nf))(
                lambda: remote(own, own, self.up.at[t], self.ch.at[t], here).wait_send()
            )
            pl.when((t >= at.z) & (at.z > 0))(
                lambda: remote(own, own, self.dn.at[t], self.ch.at[t], here).wait_send()
            )


class DpSpread:
    @staticmethod
    def sems(sizes):
        n_dp, nf, nm = sizes
        nfm, nx = nf * nm, n_dp // CORES
        dma = pltpu.SemaphoreType.DMA
        return [dma((nfm, max(nx - 1, 1))), dma((nfm, max(nx - 1, 1))), dma((nfm, nx)), dma((nfm, nx))]

    def __init__(self, at, out, sems):
        self.at, self.out = at, out
        self.xs, self.xr, self.cs, self.cr = sems

    def slot(self, x, c, f):
        return self.out.at[(x * CORES + c) * self.at.nfm + f]

    def send(self, f, src):
        at = self.at
        dst = self.slot(at.x, at.c, f)
        for k in range(1, at.nx):
            there = (((at.x + k) % at.nx) * CORES + at.c, at.z, at.y)
            remote(src, dst, self.xs.at[f, k - 1], self.xr.at[f, k - 1], there).start()
        there = (at.x * CORES + 1 - at.c, at.z, at.y)
        remote(src, dst, self.cs.at[f, 0], self.cr.at[f, 0], there).start()

    def forward(self, f):
        at = self.at
        here = (at.d, at.z, at.y)
        there = (at.x * CORES + 1 - at.c, at.z, at.y)
        for k in range(1, at.nx):
            dst = self.slot((at.x + at.nx - k) % at.nx, at.c, f)
            remote(dst, dst, self.xs.at[f, k - 1], self.xr.at[f, k - 1], here).wait_recv()
            remote(dst, dst, self.cs.at[f, k], self.cr.at[f, k], there).start()

    def landed(self):
        at = self.at
        here = (at.d, at.z, at.y)
        for f in range(at.nfm):
            for k in range(at.nx):
                dst = self.slot((at.x + at.nx - k) % at.nx, 1 - at.c, f)
                remote(dst, dst, self.cs.at[f, k], self.cr.at[f, k], here).wait_recv()

    def finish(self):
        at = self.at
        here = (at.d, at.z, at.y)
        for f in range(at.nfm):
            for k in range(at.nx):
                dst = self.slot(at.x, at.c, f)
                remote(dst, dst, self.cs.at[f, k], self.cr.at[f, k], here).wait_send()
            for k in range(1, at.nx):
                dst = self.slot(at.x, at.c, f)
                remote(dst, dst, self.xs.at[f, k - 1], self.xr.at[f, k - 1], here).wait_send()


class Early:
    @staticmethod
    def sems(sizes, count):
        nfm = sizes[1] * sizes[2]
        dma = pltpu.SemaphoreType.DMA
        return [dma((count, nfm - 1)), dma((count, nfm - 1)), dma((count,))]

    def __init__(self, at, moments, out, sems):
        self.at, self.moments, self.out = at, moments, out
        self.ss, self.rs, self.ls = sems
        self.group = out.shape[3]

    def part(self, k, f):
        matrices = self.moments[0].shape[0]
        cols = pl.ds(pl.multiple_of(f * self.group, self.group), self.group)
        return self.moments[k // matrices].at[k % matrices, :, cols]

    def start(self, k):
        at = self.at
        mine = self.out.at[k, at.f]
        for j in range(1, at.nfm):
            f = (at.f + j) % at.nfm
            remote(self.part(k, f), mine, self.ss.at[k, j - 1], self.rs.at[k, j - 1], at.fm_device(f)).start()
        pltpu.make_async_copy(self.part(k, at.f), mine, self.ls.at[k]).start()

    def finish(self, k):
        at = self.at
        for j in range(1, at.nfm):
            f = (at.f + at.nfm - j) % at.nfm
            dst = self.out.at[k, f]
            remote(dst, dst, self.ss.at[k, j - 1], self.rs.at[k, j - 1], at.fm_device(f)).wait()
        pltpu.make_async_copy(self.part(k, at.f), self.out.at[k, at.f], self.ls.at[k]).wait()


def inputs_kernel(sizes, early_count, tok_ref, w_ref, *refs):
    moments, refs = refs[:2], refs[2:]
    if early_count:
        (xall_ref, wall_ref, early_ref), refs = refs[:3], refs[3:]
    else:
        (xall_ref, wall_ref), refs = refs[:2], refs[2:]
    as_sem, ar_sem, wl_sem, *sems = refs
    at = Where(sizes)
    early = Early(at, moments, early_ref, sems[10:13]) if early_count else None
    group = wall_ref.shape[3]
    plane = PlaneSpread(at, tok_ref, xall_ref, sems[:6])
    along = DpSpread(at, wall_ref, sems[6:10])
    at.greet()
    mine = wall_ref.at[at.d * at.nfm + at.f]

    def columns(f):
        return w_ref.at[0:3, :, pl.ds(pl.multiple_of(f * group, group), group)]

    for j in range(1, at.nfm):
        f = (at.f + j) % at.nfm
        remote(columns(f), mine, as_sem.at[j - 1], ar_sem.at[j - 1], at.fm_device(f)).start()
    plane.begin()
    local = pltpu.make_async_copy(columns(at.f), mine, wl_sem.at[0])
    local.start()
    along.send(at.f, columns(at.f))
    for j in range(1, at.nfm):
        f = (at.f + at.nfm - j) % at.nfm
        dst = wall_ref.at[at.d * at.nfm + f]
        remote(dst, dst, as_sem.at[j - 1], ar_sem.at[j - 1], at.fm_device(f)).wait_recv()
        along.send(f, dst)
    for s in range(1, at.nf):
        plane.step(s)
        if s == 1:
            for j in range(at.nfm):
                along.forward((at.f + at.nfm - j) % at.nfm)
        for k in range(early_count):
            if min(k // EARLY_STEP + 1, at.nf - 1) == s:
                early.start(k)
    for s in range(at.nf):
        plane.sides(s)
    along.landed()
    along.finish()
    plane.finish()
    local.wait()
    for k in range(early_count):
        early.finish(k)
    for j in range(1, at.nfm):
        remote(mine, mine, as_sem.at[j - 1], ar_sem.at[j - 1], at.fm_device(at.f)).wait_send()


def share_inputs(sizes, tokens_in, old_weights, old_first, old_second, early_count=0):
    n_dp, nf, nm = sizes
    nfm = nf * nm
    rows, columns = old_weights.shape[1:]
    dma = pltpu.SemaphoreType.DMA
    return pl.pallas_call(
        functools.partial(inputs_kernel, sizes, early_count),
        out_shape=(
            jax.ShapeDtypeStruct((nfm,) + tokens_in.shape, tokens_in.dtype),
            jax.ShapeDtypeStruct((n_dp * nfm, 3, rows, columns // nfm), old_weights.dtype),
        )
        + ((jax.ShapeDtypeStruct((early_count, nfm, rows, columns // nfm), old_first.dtype),) if early_count else ()),
        in_specs=[ANY, ANY, ANY, ANY],
        out_specs=(ANY, ANY, ANY) if early_count else (ANY, ANY),
        scratch_shapes=[dma((nfm - 1,)), dma((nfm - 1,)), dma((1,))]
        + PlaneSpread.sems(sizes)
        + DpSpread.sems(sizes)
        + (Early.sems(sizes, early_count) if early_count else []),
        compiler_params=pltpu.CompilerParams(collective_id=0, has_side_effects=True),
        name="share_inputs",
    )(tokens_in, old_weights, old_first, old_second)


def outputs_kernel(sizes, att_ref, w_ref, aall_ref, oall_ref, *sems):
    at = Where(sizes)
    plane = PlaneSpread(at, att_ref, aall_ref, sems[:6])
    along = DpSpread(at, oall_ref, sems[12:16])
    wide = PlaneSpread(at, w_ref.at[3], oall_ref, sems[6:12], at.d * at.nfm, along.send)
    at.greet()
    plane.begin()
    wide.begin()
    for s in range(1, at.nf):
        plane.step(s)
        wide.step(s)
    for s in range(at.nf):
        plane.sides(s)
        wide.sides(s)
    for f in range(at.nfm):
        along.forward((at.f + f) % at.nfm)
    along.landed()
    along.finish()
    plane.finish()
    wide.finish()


def share_outputs(sizes, attended, old_weights):
    n_dp, nf, nm = sizes
    nfm = nf * nm
    rows, columns = old_weights.shape[1:]
    return pl.pallas_call(
        functools.partial(outputs_kernel, sizes),
        out_shape=(
            jax.ShapeDtypeStruct((nfm,) + attended.shape, attended.dtype),
            jax.ShapeDtypeStruct((n_dp * nfm, rows, columns), old_weights.dtype),
        ),
        in_specs=[ANY, ANY],
        out_specs=(ANY, ANY),
        scratch_shapes=PlaneSpread.sems(sizes) + PlaneSpread.sems(sizes) + DpSpread.sems(sizes),
        compiler_params=pltpu.CompilerParams(collective_id=1, has_side_effects=True),
        name="share_outputs",
    )(attended, old_weights)


def keep_residue(full, wide_ref, chosen_ref, res, dp_count):
    rows = wide_ref.shape[1] // dp_count
    for c in range(wide_ref.shape[0]):
        at = slice(c * LANES, (c + 1) * LANES)
        wide_ref[c] = full[:, at].astype(jnp.float32)
        chosen_ref[:, at] = wide_ref[c, pl.ds(res, rows, stride=dp_count), :].astype(chosen_ref.dtype)


def attend_kernel(
    dp_count, place_ref, res_ref, x_ref, wall_ref, segr_ref, segc_ref, att_ref, kept_ref, wbuf, wide, q_ref, k_ref, v_ref, sems
):
    blocks, _, rows, _ = wall_ref.shape
    seq, group = att_ref.shape

    def fetch(p):
        at = pl.ds(pl.multiple_of(place_ref[p] * rows, rows), rows)
        return pltpu.make_async_copy(wall_ref.at[p], wbuf.at[:, at], sems.at[p])

    for p in range(blocks):
        fetch(p).start()
    for p in range(blocks):
        fetch(p).wait()
    tile = 256

    def project(i, carry):
        at = pl.ds(pl.multiple_of(i * tile, tile), tile)
        x = x_ref[at, :]
        for m, ref in enumerate((q_ref, k_ref, v_ref)):
            ref[at, :] = jnp.dot(x, wbuf[m], preferred_element_type=jnp.float32).astype(jnp.bfloat16)
        return carry

    lax.fori_loop(0, seq // tile, project, 0)
    scale = 1.0 / math.sqrt(HD)
    for i in range(seq // tile):
        low, high = i * tile, (i + 1) * tile
        rowid = lax.broadcasted_iota(jnp.int32, (tile, high), 0) + low
        colid = lax.broadcasted_iota(jnp.int32, (tile, high), 1)
        allowed = (rowid >= colid) & (segc_ref[low:high, :1] == segr_ref[:1, :high])
        for h in range(group // HD):
            cols = slice(h * HD, (h + 1) * HD)
            scores = lax.dot_general(
                q_ref[low:high, cols], k_ref[:high, cols], (((1,), (1,)), ((), ())), preferred_element_type=jnp.float32
            )
            scores = jnp.where(allowed, scores * scale, -1e30)
            expo = jnp.exp(scores - jnp.max(scores, axis=1, keepdims=True))
            soft = (expo / jnp.sum(expo, axis=1, keepdims=True)).astype(jnp.bfloat16)
            out = jnp.dot(soft, v_ref[:high, cols], preferred_element_type=jnp.float32)
            att_ref[low:high, cols] = out.astype(jnp.bfloat16)
    for m in range(3):
        keep_residue(wbuf.at[m], wide, kept_ref.at[m], res_ref[0], dp_count)


def attend(dp_count, place, own_res, x_full, wall, segments):
    seq, width = x_full.shape
    blocks, _, rows, group = wall.shape
    bf16, f32 = jnp.bfloat16, jnp.float32
    return pl.pallas_call(
        functools.partial(attend_kernel, dp_count),
        out_shape=(
            jax.ShapeDtypeStruct((seq, group), bf16),
            jax.ShapeDtypeStruct((3, width // dp_count, group), bf16),
        ),
        in_specs=[SMEM, SMEM, VMEM, ANY, VMEM, VMEM],
        out_specs=(VMEM, VMEM),
        scratch_shapes=[
            pltpu.VMEM((3, width, group), bf16),
            pltpu.VMEM((group // LANES, width, LANES), f32),
            pltpu.VMEM((seq, group), bf16),
            pltpu.VMEM((seq, group), bf16),
            pltpu.VMEM((seq, group), bf16),
            pltpu.SemaphoreType.DMA((blocks,)),
        ],
        compiler_params=pltpu.CompilerParams(vmem_limit_bytes=VMEM_MOST),
        cost_estimate=pl.CostEstimate(flops=8 * 10**9, bytes_accessed=3 * 10**7, transcendentals=10**6),
        name="attend",
    )(place, own_res, x_full, wall, segments[None, :], segments[:, None])


def head_kernel(
    dp_count, place_ref, res_ref, f_ref, x_ref, a_ref, oall_ref, hw_ref, gain_ref, tgt_ref, out_ref, kept_ref,
    obuf, hbuf, wide, abuf, hid, norm, sems, hsem,
):
    blocks, rows, columns = oall_ref.shape
    tile, width = x_ref.shape
    fm_count, _, group = a_ref.shape
    vocab = hw_ref.shape[1]
    chunk = 256

    def fetch(p):
        at = pl.ds(pl.multiple_of(place_ref[p] * rows, rows), rows)
        return pltpu.make_async_copy(oall_ref.at[p], obuf.at[at], sems.at[p])

    def fetch_head():
        return pltpu.make_async_copy(hw_ref, hbuf, hsem.at[0])

    @pl.when(pl.program_id(0) == 0)
    def _():
        for p in range(blocks):
            fetch(p).start()
        fetch_head().start()
        for p in range(blocks):
            fetch(p).wait()

    for f in range(fm_count):
        abuf[:, f * group : (f + 1) * group] = a_ref[f]

    def hidden(i, total):
        at = pl.ds(pl.multiple_of(i * chunk, chunk), chunk)
        part = lax.dot_general(
            abuf[...], obuf[at, :], (((1,), (1,)), ((), ())), preferred_element_type=jnp.float32
        )
        part = part + x_ref[:, at].astype(jnp.float32)
        hid[:, at] = part
        return total + jnp.sum(part * part, axis=1, keepdims=True)

    total = lax.fori_loop(0, width // chunk, hidden, jnp.zeros((tile, 1), jnp.float32))
    scale = lax.rsqrt(total / width + 1e-05)

    def normed(i, carry):
        at = pl.ds(pl.multiple_of(i * chunk, chunk), chunk)
        norm[:, at] = (hid[:, at] * scale * gain_ref[:, at]).astype(jnp.bfloat16)
        return carry

    lax.fori_loop(0, width // chunk, normed, 0)

    @pl.when(pl.program_id(0) == 0)
    def _():
        fetch_head().wait()
        own = pl.ds(pl.multiple_of(f_ref[0] * group, group), group)
        keep_residue(obuf[:, own], wide, kept_ref, res_ref[0], dp_count)

    local = tgt_ref[:, :1] - f_ref[0] * vocab
    lane = lax.broadcasted_iota(jnp.int32, (tile, chunk), 1)

    def score(i, carry):
        top, total, picked = carry
        at = pl.ds(pl.multiple_of(i * chunk, chunk), chunk)
        logits = jnp.dot(norm[...], hbuf[:, at], preferred_element_type=jnp.float32)
        higher = jnp.maximum(top, jnp.max(logits, axis=1, keepdims=True))
        total = total * jnp.exp(top - higher) + jnp.sum(jnp.exp(logits - higher), axis=1, keepdims=True)
        hit = jnp.where(lane + i * chunk == local, logits, 0.0)
        return higher, total, picked + jnp.sum(hit, axis=1, keepdims=True)

    zero = jnp.zeros((tile, 1), jnp.float32)
    top, total, picked = lax.fori_loop(0, vocab // chunk, score, (zero - 1e30, zero, zero))
    lanes = lax.broadcasted_iota(jnp.int32, (tile, 128), 1)
    out_ref[...] = jnp.where(lanes == 0, top, jnp.where(lanes == 1, total, picked))


def head_parts(dp_count, place, own_res, own_f, x_full, a_all, oall, head_weight, norm_gain, targets):
    seq, width = x_full.shape
    fm_count, _, group = a_all.shape
    blocks, rows, columns = oall.shape
    vocab = head_weight.shape[1]
    tile = 256
    bf16, f32 = jnp.bfloat16, jnp.float32
    return pl.pallas_call(
        functools.partial(head_kernel, dp_count),
        grid=(seq // tile,),
        out_shape=(
            jax.ShapeDtypeStruct((seq, 128), f32),
            jax.ShapeDtypeStruct((width // dp_count, group), bf16),
        ),
        in_specs=[
            SMEM,
            SMEM,
            SMEM,
            pl.BlockSpec((tile, width), lambda i: (i, 0)),
            pl.BlockSpec((fm_count, tile, group), lambda i: (0, i, 0)),
            ANY,
            ANY,
            pl.BlockSpec((1, width), lambda i: (0, 0)),
            pl.BlockSpec((tile, 1), lambda i: (i, 0)),
        ],
        out_specs=(
            pl.BlockSpec((tile, 128), lambda i: (i, 0)),
            pl.BlockSpec((width // dp_count, group), lambda i: (0, 0)),
        ),
        scratch_shapes=[
            pltpu.VMEM((width, columns), bf16),
            pltpu.VMEM((width, vocab), bf16),
            pltpu.VMEM((group // LANES, width, LANES), f32),
            pltpu.VMEM((tile, columns), bf16),
            pltpu.VMEM((tile, width), f32),
            pltpu.VMEM((tile, width), bf16),
            pltpu.SemaphoreType.DMA((blocks,)),
            pltpu.SemaphoreType.DMA((1,)),
        ],
        compiler_params=pltpu.CompilerParams(vmem_limit_bytes=VMEM_MOST),
        cost_estimate=pl.CostEstimate(flops=2 * 10**10, bytes_accessed=4 * 10**7, transcendentals=10**6),
        name="head_parts",
    )(place, own_res, own_f, x_full, a_all, oall, head_weight, norm_gain[None, :], targets[:, None])


def in_blocks(wall, table, holder):
    if wall.shape[-2] % 16 == 0:
        return wall, table
    ordered = jnp.take(wall, holder, axis=0, mode="clip")
    blocks, rows = ordered.shape[0], ordered.shape[-2]
    join = 16 // math.gcd(16, rows)
    middle = ordered.shape[1:-2]
    ordered = ordered.reshape((blocks // join, join) + middle + ordered.shape[-2:])
    ordered = jnp.moveaxis(ordered, 1, -3)
    ordered = ordered.reshape((blocks // join,) + middle + (join * rows, ordered.shape[-1]))
    return ordered, jnp.arange(blocks // join, dtype=jnp.int32)


def body(
    sizes,
    tokens_in,
    segment_ids,
    target_ids,
    old_weights,
    old_first,
    old_second,
    old_block,
    new_residue,
    norm_gain,
    head_weight,
):
    dp_count, nf, nm = sizes
    fm_count = nf * nm
    segments, targets, table, residues = share_tables(segment_ids, target_ids, old_block, new_residue)
    holder = inverse_of(table)
    own_f = lax.axis_index(("fsdp", "mp"))[None]
    first_sent = pack_moments(old_first, residues, fm_count)
    second_sent = pack_moments(old_second, residues, fm_count)
    first_got = lax.all_to_all(first_sent, EVERYONE, split_axis=0, concat_axis=0, tiled=True)
    second_got = lax.all_to_all(second_sent, EVERYONE, split_axis=0, concat_axis=0, tiled=True)
    x_all, wall = share_inputs(sizes, tokens_in, old_weights, old_first, old_second)
    x_full = x_all.reshape(-1, tokens_in.shape[1])
    wall, place = in_blocks(wall, table, holder)
    attended, kept = attend(dp_count, place, new_residue, x_full, wall, segments)
    a_all, oall = share_outputs(sizes, attended, old_weights)
    oall, place = in_blocks(oall, table, holder)
    parts, kept_out = head_parts(
        dp_count, place, new_residue, own_f, x_full, a_all, oall, head_weight, norm_gain, targets
    )
    loss = joint_loss(parts[:, :3].T)
    new_weights = jnp.concatenate([kept, kept_out[None]])
    new_first = unpack_moments(first_got, table, holder)
    new_second = unpack_moments(second_got, table, holder)
    return (new_weights, new_first, new_second, loss)


class Moments:
    @staticmethod
    def sems(sizes, pieces, halves):
        n_dp, nf, nm = sizes
        nfm = nf * nm
        dma = pltpu.SemaphoreType.DMA
        return [
            dma((pieces, nfm, halves)),
            dma((pieces, nfm, halves)),
            dma((pieces, n_dp)),
            dma((pieces, n_dp)),
        ]

    def __init__(self, at, early_count, moments, early, res, land, sent, got, sems):
        self.at, self.early_count, self.moments, self.early = at, early_count, moments, early
        self.res, self.land, self.sent, self.got = res, land, sent, got
        self.as_, self.ar, self.bs, self.br = sems
        self.matrices = moments[0].shape[0]
        self.nfm, self.halves = land[0].shape[:2]
        self.pair = sent.shape[3]

    def part(self, k, f, h):
        at = pl.ds(pl.multiple_of((f * self.halves + h) * LANES, LANES), LANES)
        return self.moments[k // self.matrices].at[k % self.matrices, :, at]

    def local(self, k, f, h):
        if k < self.early_count:
            src = self.early.at[k, f, :, h * LANES : (h + 1) * LANES]
        else:
            src = self.part(k, f, h)
        return pltpu.make_async_copy(src, self.land[k].at[f, h], self.ar.at[k, f, h])

    def start(self, k):
        at = self.at
        if k < self.early_count:
            for f in range(self.nfm):
                for h in range(self.halves):
                    self.local(k, f, h).start()
            return
        for j in range(1, self.nfm):
            f = (at.f + j) % self.nfm
            for h in range(self.halves):
                remote(
                    self.part(k, f, h), self.land[k].at[at.f, h], self.as_.at[k, f, h], self.ar.at[k, at.f, h], at.fm_device(f)
                ).start()
        for h in range(self.halves):
            self.local(k, at.f, h).start()

    def pick(self, k):
        at = self.at
        if k < self.early_count:
            for f in range(self.nfm):
                for h in range(self.halves):
                    self.local(k, f, h).wait()
        else:
            for j in range(1, self.nfm):
                f = (at.f + self.nfm - j) % self.nfm
                for h in range(self.halves):
                    dst = self.land[k].at[f, h]
                    remote(dst, dst, self.as_.at[k, f, h], self.ar.at[k, f, h], at.fm_device(f)).wait_recv()
            for h in range(self.halves):
                self.local(k, at.f, h).wait()

        def rows_of(f, carry):
            for i in range(at.n_dp):
                for h in range(self.halves):
                    rows = self.land[k][f, h, pl.ds(self.res[i], self.pair, stride=at.n_dp), :]
                    self.sent[k, i, f, :, h * LANES : (h + 1) * LANES] = rows
            return carry

        lax.fori_loop(0, self.nfm, rows_of, 0)

    def target(self, k, d):
        return self.got.at[k // self.matrices, pl.ds(d * self.nfm, self.nfm), k % self.matrices]

    def own(self, k):
        return pltpu.make_async_copy(self.sent.at[k, self.at.d], self.target(k, self.at.d), self.br.at[k, self.at.d])

    def send(self, k):
        at = self.at
        for j in range(1, at.n_dp):
            i = (at.d + j) % at.n_dp
            remote(
                self.sent.at[k, i], self.target(k, at.d), self.bs.at[k, i], self.br.at[k, at.d], (i, at.z, at.y)
            ).start()
        self.own(k).start()

    def finish(self, k):
        at = self.at
        for j in range(1, at.n_dp):
            i = (at.d + at.n_dp - j) % at.n_dp
            dst = self.target(k, i)
            remote(dst, dst, self.bs.at[k, i], self.br.at[k, i], (i, at.z, at.y)).wait_recv()
        self.own(k).wait()
        for j in range(1, at.n_dp):
            i = (at.d + j) % at.n_dp
            remote(
                self.sent.at[k, i], self.target(k, at.d), self.bs.at[k, i], self.br.at[k, at.d], (i, at.z, at.y)
            ).wait_send()
        if k >= self.early_count:
            for j in range(1, self.nfm):
                f = (at.f + j) % self.nfm
                for h in range(self.halves):
                    src = self.part(k, f, h)
                    remote(src, src, self.as_.at[k, f, h], self.ar.at[k, f, h], at.fm_device(f)).wait_send()


def final_kernel(
    sizes, early_count, holder_ref, res_ref, att_ref, w_ref, first_ref, second_ref, early_ref, x_ref, hw_ref, gain_ref,
    tgt_ref, out_ref, kept_ref, got_ref, owall, obuf, xbuf, hbuf, abuf, hid, norm, sent, wide, wsem, *refs,
):
    at = Where(sizes)
    blocks, rows, columns = owall.shape
    seq, width = xbuf.shape
    _, _, group = abuf.shape
    vocab = hbuf.shape[1]
    tiles = seq // ROW_TILE
    chunk = 256
    pieces = sent.shape[0]
    land, sems = refs[:pieces], refs[pieces:]
    step = len(PlaneSpread.sems(sizes))
    planes = []
    for i in range(tiles):
        own = slice(i * ROW_TILE, (i + 1) * ROW_TILE)
        planes.append(
            PlaneSpread(at, att_ref.at[own], abuf, sems[i * step : (i + 1) * step], rows=own)
        )
    sems = sems[tiles * step :]
    along = DpSpread(at, owall, sems[step : step + 4])
    whole = PlaneSpread(at, w_ref.at[3], owall, sems[:step], at.d * at.nfm, along.send)
    moments = Moments(at, early_count, (first_ref, second_ref), early_ref, res_ref, land, sent, got_ref, sems[step + 4 :])
    loads = [pltpu.make_async_copy(x_ref, xbuf, wsem.at[0]), pltpu.make_async_copy(hw_ref, hbuf, wsem.at[1])]
    at.greet(diagonal=True)
    for plane in planes:
        plane.begin()
    whole.begin()
    for k in range(early_count):
        moments.start(k)
    for load in loads:
        load.start()
    waiting = list(range(early_count, pieces))
    flying, picked = list(range(early_count)), []

    def launch(count=1):
        for _ in range(count):
            if waiting:
                k = waiting.pop(0)
                moments.start(k)
                flying.append(k)

    def turn(count=1):
        for _ in range(count):
            if flying:
                k = flying.pop(0)
                moments.pick(k)
                picked.append(k)
                if len(picked) > 1:
                    moments.send(picked[-2])
            elif picked and picked[-1] != pieces:
                moments.send(picked[-1])
                picked.append(pieces)

    turn(early_count)
    launch()
    for s in range(1, at.nf):
        for plane in planes:
            plane.step(s)
        whole.step(s)
        launch()
    for s in range(at.nf):
        for plane in planes:
            plane.sides(s)
        whole.sides(s)
    for f in range(at.nfm):
        along.forward((at.f + f) % at.nfm)
    launch(pieces)
    turn(2)
    along.landed()
    own = whole.slot(at.z, at.y)
    pltpu.make_async_copy(whole.own, own, whole.lc.at[0]).wait()

    def order(b, carry):
        obuf[pl.ds(pl.multiple_of(b * rows, rows), rows), :] = owall[holder_ref[b]]
        return carry

    lax.fori_loop(0, blocks, order, 0)
    for load in loads:
        load.wait()
    for plane in planes:
        pltpu.make_async_copy(plane.own, plane.slot(at.z, at.y), plane.lc.at[0]).wait()
    lane = lax.broadcasted_iota(jnp.int32, (ROW_TILE, chunk), 1)
    lanes = lax.broadcasted_iota(jnp.int32, (ROW_TILE, LANES), 1)

    def one_tile(t, carry):
        here = pl.ds(pl.multiple_of(t * ROW_TILE, ROW_TILE), ROW_TILE)

        def hidden(i, total):
            cols = pl.ds(pl.multiple_of(i * chunk, chunk), chunk)
            part = xbuf[here, cols].astype(jnp.float32)
            for f in range(at.nfm):
                part += lax.dot_general(
                    abuf[f, here, :],
                    obuf[cols, f * group : (f + 1) * group],
                    (((1,), (1,)), ((), ())),
                    preferred_element_type=jnp.float32,
                )
            hid[:, cols] = part
            return total + jnp.sum(part * part, axis=1, keepdims=True)

        total = lax.fori_loop(0, width // chunk, hidden, jnp.zeros((ROW_TILE, 1), jnp.float32))
        scale = lax.rsqrt(total / width + 1e-05)

        def normed(i, carry):
            cols = pl.ds(pl.multiple_of(i * chunk, chunk), chunk)
            norm[:, cols] = (hid[:, cols] * scale * gain_ref[:, cols]).astype(jnp.bfloat16)
            return carry

        lax.fori_loop(0, width // chunk, normed, 0)
        local = tgt_ref[here, :1] - at.f * vocab

        def score(i, carry):
            top, total, picked = carry
            cols = pl.ds(pl.multiple_of(i * chunk, chunk), chunk)
            logits = jnp.dot(norm[...], hbuf[:, cols], preferred_element_type=jnp.float32)
            higher = jnp.maximum(top, jnp.max(logits, axis=1, keepdims=True))
            total = total * jnp.exp(top - higher) + jnp.sum(jnp.exp(logits - higher), axis=1, keepdims=True)
            hit = jnp.where(lane + i * chunk == local, logits, 0.0)
            return higher, total, picked + jnp.sum(hit, axis=1, keepdims=True)

        zero = jnp.zeros((ROW_TILE, 1), jnp.float32)
        top, total, picked = lax.fori_loop(0, vocab // chunk, score, (zero - 1e30, zero, zero))
        out_ref[here, :] = jnp.where(lanes == 0, top, jnp.where(lanes == 1, total, picked))
        return carry

    for t in range(tiles):
        lax.fori_loop(t, t + 1, one_tile, 0)
        turn()
    part_rows = wide.shape[0]
    for c in range(group // LANES):
        cols = pl.ds(pl.multiple_of(at.f * group + c * LANES, LANES), LANES)
        for i in range(width // part_rows):
            wide[...] = obuf[i * part_rows : (i + 1) * part_rows, cols].astype(jnp.float32)
            kept = wide[pl.ds(res_ref[at.d], part_rows // at.n_dp, stride=at.n_dp), :]
            kept_rows = part_rows // at.n_dp
            kept_ref[i * kept_rows : (i + 1) * kept_rows, c * LANES : (c + 1) * LANES] = kept.astype(kept_ref.dtype)
    turn(pieces)
    turn(1)
    along.finish()
    for plane in planes + [whole]:
        plane.sent()
    for k in range(pieces):
        moments.finish(k)


def finish_all(sizes, early_count, holder, residues, attended, old_weights, old_first, old_second, early, x_full,
               head_weight, norm_gain, targets):
    n_dp, nf, nm = sizes
    nfm = nf * nm
    matrices, rows, columns = old_weights.shape
    seq, width = x_full.shape
    vocab = head_weight.shape[1]
    group, devices, pair_rows = columns // nfm, n_dp * nfm, rows // n_dp
    halves, pieces = group // LANES, 2 * matrices
    bf16, f32 = jnp.bfloat16, jnp.float32
    plane_sems = PlaneSpread.sems(sizes)
    return pl.pallas_call(
        functools.partial(final_kernel, sizes, early_count),
        out_shape=(
            jax.ShapeDtypeStruct((seq, LANES), f32),
            jax.ShapeDtypeStruct((width // n_dp, group), bf16),
            jax.ShapeDtypeStruct((2, devices, matrices, pair_rows, group), f32),
        ),
        in_specs=[SMEM, SMEM] + [ANY] * 7 + [VMEM, VMEM],
        out_specs=(VMEM, VMEM, ANY),
        scratch_shapes=[
            pltpu.VMEM((devices, rows, columns), bf16),
            pltpu.VMEM((width, columns), bf16),
            pltpu.VMEM((seq, width), bf16),
            pltpu.VMEM((width, vocab), bf16),
            pltpu.VMEM((nfm, seq, group), bf16),
            pltpu.VMEM((ROW_TILE, width), f32),
            pltpu.VMEM((ROW_TILE, width), bf16),
            pltpu.VMEM((pieces, n_dp, nfm, pair_rows, group), f32),
            pltpu.VMEM((width // 4, LANES), f32),
            pltpu.SemaphoreType.DMA((2,)),
        ]
        + [pltpu.VMEM((nfm, halves, rows, LANES), f32)] * pieces
        + plane_sems * (seq // ROW_TILE + 1)
        + DpSpread.sems(sizes)
        + Moments.sems(sizes, pieces, halves),
        compiler_params=pltpu.CompilerParams(
            collective_id=2, has_side_effects=True, vmem_limit_bytes=63 * 1024 * 1024
        ),
        cost_estimate=pl.CostEstimate(flops=2 * 10**10, bytes_accessed=4 * 10**7, transcendentals=10**6),
        name="finish_all",
    )(holder, residues, attended, old_weights, old_first, old_second, early, x_full, head_weight, norm_gain[None, :],
      targets[:, None])


def body_close(
    sizes,
    tokens_in,
    segment_ids,
    target_ids,
    old_weights,
    old_first,
    old_second,
    old_block,
    new_residue,
    norm_gain,
    head_weight,
):
    dp_count = sizes[0]
    segments, targets, table, residues = share_tables(segment_ids, target_ids, old_block, new_residue)
    holder = inverse_of(table)
    x_all, wall, early = share_inputs(sizes, tokens_in, old_weights, old_first, old_second, EARLY)
    x_full = x_all.reshape(-1, tokens_in.shape[1])
    attended, kept = attend(dp_count, table, new_residue, x_full, wall, segments)
    parts, kept_out, got = finish_all(
        sizes, EARLY, holder, residues, attended, old_weights, old_first, old_second, early, x_full, head_weight,
        norm_gain, targets,
    )
    loss = joint_loss(parts[:, :3].T)
    new_weights = jnp.concatenate([kept, kept_out[None]])
    new_first, new_second = (unpack_moments(got, table, holder, q) for q in range(2))
    return (new_weights, new_first, new_second, loss)


def solution(mesh):
    placed = (
        P(EVERYONE, None),
        P(EVERYONE),
        P(EVERYONE),
        P(None, EVERYONE, None),
        P(None, EVERYONE, None),
        P(None, EVERYONE, None),
        P(EVERYONE),
        P("dp"),
        P(),
        P(None, ("fsdp", "mp")),
    )
    sizes = tuple(mesh.shape[name] for name in EVERYONE)

    def step(*args):
        rows, columns = args[3].shape[1:]
        seq = args[0].shape[0] * sizes[1] * sizes[2]
        close = rows % 16 == 0 and (rows // sizes[0]) % 8 == 0 and seq <= 1024 and columns <= 2048
        return (body_close if close else body)(sizes, *args)

    return jax.shard_map(
        step,
        mesh=mesh,
        in_specs=placed,
        out_specs=(
            P(None, "dp", ("fsdp", "mp")),
            P(None, "dp", ("fsdp", "mp")),
            P(None, "dp", ("fsdp", "mp")),
            P(EVERYONE),
        ),
        check_vma=False,
    )
```

```python
import functools
import math

import jax
import jax.numpy as jnp
from jax import lax
from jax.experimental import pallas as pl
from jax.experimental.pallas import tpu as pltpu
from jax.sharding import PartitionSpec as P

HD = 128
LANES = 128
MESH = pl.DeviceIdType.MESH
ANY = pl.BlockSpec(memory_space=pl.ANY)
SMEM = pl.BlockSpec(memory_space=pltpu.SMEM)
VMEM = pl.BlockSpec(memory_space=pltpu.VMEM)
EVERYONE = ("dp", "fsdp", "mp")
VMEM_MOST = 60 * 1024 * 1024
CORES = 2
EARLY = 2
EARLY_STEPS = 2
EARLY_SIDES = 1
LATE_STEPS = 1
LATE_SIDES = 1
TURNS = 0
TURN_FROM = 9
TURNS_AFTER = 3
IN_CHUNKS = 4
ROW_TILE = 256


def inverse_of(table):
    total_count = table.shape[0]
    places = jnp.arange(total_count, dtype=jnp.int32)
    return jnp.sum(jnp.where(table[None, :] == places[:, None], places[None, :], 0), axis=1)


def share_tables(segment_ids, target_ids, old_block, new_residue):
    own = jnp.concatenate([segment_ids, target_ids, old_block, new_residue])
    rows = jnp.broadcast_to(own[None, None], (lax.axis_size(EVERYONE), 1, own.shape[0]))
    rows = lax.all_to_all(rows, EVERYONE, split_axis=0, concat_axis=0, tiled=True)[:, 0]
    count = segment_ids.shape[0]
    fm_count = lax.axis_size(("fsdp", "mp"))
    here = lax.dynamic_slice_in_dim(rows, lax.axis_index("dp") * fm_count, fm_count)
    segments = here[:, :count].reshape(-1)
    targets = here[:, count : 2 * count].reshape(-1)
    return segments, targets, rows[:, 2 * count], rows[::fm_count, 2 * count + 1]


def joint_loss(parts):
    axes = ("fsdp", "mp")
    fm_count = lax.axis_size(axes)
    own_count = parts.shape[1] // fm_count
    parts = parts.reshape(3, fm_count, own_count).transpose(1, 0, 2)
    parts = lax.all_to_all(parts, axes, split_axis=0, concat_axis=0, tiled=True)
    tops, totals, targets = parts[:, 0], parts[:, 1], parts[:, 2]
    joint_max = jnp.max(tops, axis=0)
    joint_total = jnp.sum(totals * jnp.exp(tops - joint_max[None]), axis=0)
    return joint_max + jnp.log(joint_total) - jnp.sum(targets, axis=0)


def pack_kernel(dp_count, fm_count, res_ref, old_ref, sent_ref, lanes):
    rows, columns = old_ref.shape[1:]
    pair_rows, group = rows // dp_count, columns // fm_count
    for c in range(columns // LANES):
        lanes[c] = old_ref[0, :, c * LANES : (c + 1) * LANES]
    for i in range(dp_count):
        for c in range(columns // LANES):
            f, at = divmod(c * LANES, group)
            chosen = lanes[c, pl.ds(res_ref[i], pair_rows, stride=dp_count), :]
            sent_ref[i * fm_count + f, 0, :, at : at + LANES] = chosen


def pack_moments(stored, residues, fm_count):
    matrices, row_count, columns = stored.shape
    dp_count = residues.shape[0]
    pair_rows, group = row_count // dp_count, columns // fm_count
    devices = dp_count * fm_count
    if pair_rows % 8:
        split_rows = stored.reshape(matrices, pair_rows, dp_count, fm_count, group)
        chosen = jnp.take(split_rows, residues, axis=2, mode="clip")
        return chosen.transpose(2, 3, 0, 1, 4).reshape(devices, matrices, pair_rows, group)
    return pl.pallas_call(
        functools.partial(pack_kernel, dp_count, fm_count),
        grid=(matrices,),
        out_shape=jax.ShapeDtypeStruct((devices, matrices, pair_rows, group), stored.dtype),
        in_specs=[SMEM, pl.BlockSpec((1, row_count, columns), lambda m: (m, 0, 0))],
        out_specs=pl.BlockSpec((devices, 1, pair_rows, group), lambda m: (0, m, 0, 0)),
        scratch_shapes=[pltpu.VMEM((columns // LANES, row_count, LANES), stored.dtype)],
        name="pack_moments",
    )(residues, stored)


def unpack_kernel(which, block_ref, got_ref, out_ref, buf, in_sems, out_sems):
    if which is not None:
        got_ref = got_ref.at[which]
    devices, _, pair_rows, _ = got_ref.shape
    for p in range(devices):
        pltpu.make_async_copy(got_ref.at[p], buf.at[p], in_sems.at[p]).start()
    for p in range(devices):
        pltpu.make_async_copy(got_ref.at[p], buf.at[p], in_sems.at[p]).wait()
        place = pl.ds(pl.multiple_of(block_ref[p] * pair_rows, pair_rows), pair_rows)
        pltpu.make_async_copy(buf.at[p], out_ref.at[:, place], out_sems.at[p]).start()
    for p in range(devices):
        place = pl.ds(pl.multiple_of(block_ref[p] * pair_rows, pair_rows), pair_rows)
        pltpu.make_async_copy(buf.at[p], out_ref.at[:, place], out_sems.at[p]).wait()


def unpack_moments(received, table, holder, which=None):
    devices, matrices, pair_rows, group = received.shape[-4:]
    if pair_rows % 8:
        ordered = jnp.take(received, holder, axis=0, mode="clip")
        return ordered.transpose(1, 0, 2, 3).reshape(matrices, devices * pair_rows, group)
    return pl.pallas_call(
        functools.partial(unpack_kernel, which),
        out_shape=jax.ShapeDtypeStruct((matrices, devices * pair_rows, group), received.dtype),
        in_specs=[SMEM, ANY],
        out_specs=ANY,
        scratch_shapes=[
            pltpu.VMEM(received.shape[-4:], received.dtype),
            pltpu.SemaphoreType.DMA((devices,)),
            pltpu.SemaphoreType.DMA((devices,)),
        ],
        name="unpack_moments",
    )(table, received)


def unpack_all_kernel(block_ref, early_ref, late_ref, kept_ref, last_ref, w_ref, first_ref, second_ref, buf, wbuf, isem, osem, wsem):
    pieces, devices, pair_rows, _ = buf.shape
    early, matrices = early_ref.shape[0], pieces // 2
    load = [
        pltpu.make_async_copy(early_ref.at[k] if k < early else late_ref.at[k - early], buf.at[k], isem.at[k])
        for k in range(pieces)
    ]
    three = [
        pltpu.make_async_copy(kept_ref, wbuf.at[0 : matrices - 1], wsem.at[0]),
        pltpu.make_async_copy(last_ref, wbuf.at[matrices - 1], wsem.at[1]),
    ]
    out = pltpu.make_async_copy(wbuf, w_ref, wsem.at[2])
    for copy in load[:matrices] + three + load[matrices:]:
        copy.start()

    def place(q, p):
        rows = pl.ds(pl.multiple_of(block_ref[p] * pair_rows, pair_rows), pair_rows)
        target = (first_ref, second_ref)[q].at[:, rows]
        return pltpu.make_async_copy(buf.at[q * matrices : (q + 1) * matrices, p], target, osem.at[q, p])

    for q in range(2):
        for k in range(q * matrices, (q + 1) * matrices):
            load[k].wait()
        for p in range(devices):
            place(q, p).start()
        if q == 0:
            for copy in three:
                copy.wait()
            out.start()
    for q in range(2):
        for p in range(devices):
            place(q, p).wait()
    out.wait()


def unpack_all(table, early, late, kept, last):
    _, devices, pair_rows, group = early.shape
    matrices = kept.shape[0] + 1
    moment = jax.ShapeDtypeStruct((matrices, devices * pair_rows, group), early.dtype)
    dma = pltpu.SemaphoreType.DMA
    return pl.pallas_call(
        unpack_all_kernel,
        out_shape=(jax.ShapeDtypeStruct((matrices,) + last.shape, last.dtype), moment, moment),
        in_specs=[SMEM, ANY, ANY, ANY, ANY],
        out_specs=(ANY, ANY, ANY),
        scratch_shapes=[
            pltpu.VMEM((2 * matrices,) + early.shape[1:], early.dtype),
            pltpu.VMEM((matrices,) + last.shape, last.dtype),
            dma((2 * matrices,)),
            dma((2, devices)),
            dma((3,)),
        ],
        name="unpack_all",
    )(table, early, late, kept, last)


def remote(src, dst, send_sem, recv_sem, device):
    return pltpu.make_async_remote_copy(
        src_ref=src,
        dst_ref=dst,
        send_sem=send_sem,
        recv_sem=recv_sem,
        device_id=device,
        device_id_type=MESH,
    )


class Where:
    def __init__(self, sizes):
        self.n_dp, self.nf, self.nm = sizes
        self.nx, self.nfm = self.n_dp // CORES, self.nf * self.nm
        self.d, self.z, self.y = (lax.axis_index(name) for name in EVERYONE)
        self.x, self.c = self.d // CORES, self.d % CORES
        self.f = self.z * self.nm + self.y

    def fm_device(self, f):
        return (self.d, f // self.nm, f % self.nm)

    def greet(self, diagonal=False):
        barrier = pltpu.get_barrier_semaphore()
        peers = [self.fm_device((self.f + j) % self.nfm) for j in range(1, self.nfm)]
        for k in range(1, self.nx):
            peers.append((((self.x + k) % self.nx) * CORES + self.c, self.z, self.y))
            if diagonal:
                peers.append((((self.x + k) % self.nx) * CORES + 1 - self.c, self.z, self.y))
        peers.append((self.x * CORES + 1 - self.c, self.z, self.y))
        for peer in peers:
            pl.semaphore_signal(barrier, inc=1, device_id=peer, device_id_type=MESH)
        pl.semaphore_wait(barrier, len(peers))


class PlaneSpread:
    @staticmethod
    def sems(sizes):
        _, nf, nm = sizes
        dma = pltpu.SemaphoreType.DMA
        return [dma((nf,)), dma((nf,)), dma((nf,)), dma((nf, nm - 1)), dma((nf, nm - 1)), dma((1,))]

    def __init__(self, at, own, out, sems, base=0, arrived=None, rows=None):
        self.at, self.own, self.out, self.base, self.rows = at, own, out, base, rows
        self.up, self.dn, self.ch, self.ys, self.yr, self.lc = sems
        self.arrived = arrived

    def slot(self, z, y):
        slot = self.base + z * self.at.nm + y
        return self.out.at[slot] if self.rows is None else self.out.at[slot, self.rows]

    def _pass(self, zb, src, up, down):
        at = self.at
        dst = self.slot(zb, at.y)
        if up:
            pl.when(at.z + 1 < at.nf)(
                lambda: remote(src, dst, self.up.at[zb], self.ch.at[zb], (at.d, at.z + 1, at.y)).start()
            )
        if down:
            pl.when(at.z > 0)(
                lambda: remote(src, dst, self.dn.at[zb], self.ch.at[zb], (at.d, at.z - 1, at.y)).start()
            )
        for j in range(1, at.nm):
            there = (at.d, at.z, (at.y + j) % at.nm)
            remote(src, dst, self.ys.at[zb, j - 1], self.yr.at[zb, j - 1], there).start()
        if self.arrived:
            self.arrived(zb * at.nm + at.y, src)

    def begin(self):
        at = self.at
        self._pass(at.z, self.own, True, True)
        pltpu.make_async_copy(self.own, self.slot(at.z, at.y), self.lc.at[0]).start()

    def step(self, s):
        at = self.at

        def below():
            zb = at.z - s
            dst = self.slot(zb, at.y)
            remote(dst, dst, self.up.at[zb], self.ch.at[zb], (at.d, at.z, at.y)).wait_recv()
            self._pass(zb, dst, True, False)

        def above():
            zb = at.z + s
            dst = self.slot(zb, at.y)
            remote(dst, dst, self.dn.at[zb], self.ch.at[zb], (at.d, at.z, at.y)).wait_recv()
            self._pass(zb, dst, False, True)

        pl.when(at.z - s >= 0)(below)
        pl.when(at.z + s < at.nf)(above)

    def side(self, zb):
        at = self.at
        for j in range(1, at.nm):
            source = (at.y + at.nm - j) % at.nm
            dst = self.slot(zb, source)
            remote(dst, dst, self.ys.at[zb, j - 1], self.yr.at[zb, j - 1], (at.d, at.z, at.y)).wait_recv()
            if self.arrived:
                self.arrived(zb * at.nm + source, dst)

    def sides(self, s):
        at = self.at
        if s == 0:
            self.side(at.z)
        else:
            pl.when(at.z - s >= 0)(lambda: self.side(at.z - s))
            pl.when(at.z + s < at.nf)(lambda: self.side(at.z + s))

    def finish(self):
        own = self.slot(self.at.z, self.at.y)
        pltpu.make_async_copy(self.own, own, self.lc.at[0]).wait()
        self.sent()

    def sent(self):
        at = self.at
        own = self.slot(at.z, at.y)
        here = (at.d, at.z, at.y)
        for t in range(at.nf):
            for j in range(1, at.nm):
                remote(own, own, self.ys.at[t, j - 1], self.yr.at[t, j - 1], here).wait_send()
            pl.when((t <= at.z) & (at.z + 1 < at.nf))(
                lambda: remote(own, own, self.up.at[t], self.ch.at[t], here).wait_send()
            )
            pl.when((t >= at.z) & (at.z > 0))(
                lambda: remote(own, own, self.dn.at[t], self.ch.at[t], here).wait_send()
            )


def plane_chunks(at, own, out, sems, rows):
    step = len(PlaneSpread.sems((1, 1, 2)))
    planes = []
    for low in range(0, own.shape[0], rows):
        here = slice(low, low + rows)
        planes.append(PlaneSpread(at, own.at[here], out, sems[:step], rows=here))
        sems = sems[step:]
    return planes, sems


class DpSpread:
    @staticmethod
    def sems(sizes):
        n_dp, nf, nm = sizes
        nfm, nx = nf * nm, n_dp // CORES
        dma = pltpu.SemaphoreType.DMA
        return [dma((nfm, max(nx - 1, 1))), dma((nfm, max(nx - 1, 1))), dma((nfm, nx)), dma((nfm, nx))]

    def __init__(self, at, out, sems):
        self.at, self.out = at, out
        self.xs, self.xr, self.cs, self.cr = sems

    def slot(self, x, c, f):
        return self.out.at[(x * CORES + c) * self.at.nfm + f]

    def send(self, f, src):
        at = self.at
        dst = self.slot(at.x, at.c, f)
        for k in range(1, at.nx):
            there = (((at.x + k) % at.nx) * CORES + at.c, at.z, at.y)
            remote(src, dst, self.xs.at[f, k - 1], self.xr.at[f, k - 1], there).start()
        there = (at.x * CORES + 1 - at.c, at.z, at.y)
        remote(src, dst, self.cs.at[f, 0], self.cr.at[f, 0], there).start()

    def forward(self, f):
        at = self.at
        here = (at.d, at.z, at.y)
        there = (at.x * CORES + 1 - at.c, at.z, at.y)
        for k in range(1, at.nx):
            dst = self.slot((at.x + at.nx - k) % at.nx, at.c, f)
            remote(dst, dst, self.xs.at[f, k - 1], self.xr.at[f, k - 1], here).wait_recv()
            remote(dst, dst, self.cs.at[f, k], self.cr.at[f, k], there).start()

    def landed(self):
        at = self.at
        here = (at.d, at.z, at.y)
        for f in range(at.nfm):
            for k in range(at.nx):
                dst = self.slot((at.x + at.nx - k) % at.nx, 1 - at.c, f)
                remote(dst, dst, self.cs.at[f, k], self.cr.at[f, k], here).wait_recv()

    def finish(self):
        at = self.at
        here = (at.d, at.z, at.y)
        for f in range(at.nfm):
            for k in range(at.nx):
                dst = self.slot(at.x, at.c, f)
                remote(dst, dst, self.cs.at[f, k], self.cr.at[f, k], here).wait_send()
            for k in range(1, at.nx):
                dst = self.slot(at.x, at.c, f)
                remote(dst, dst, self.xs.at[f, k - 1], self.xr.at[f, k - 1], here).wait_send()


class Drip:
    def __init__(self, start, pieces, count):
        self.start = start
        self.left = [(k, j) for k in pieces for j in range(count)]
        self.full = []
        self.count = count

    def some(self, number):
        for _ in range(min(number, len(self.left))):
            k, j = self.left.pop(0)
            self.start(k, j)
            if j == self.count - 1:
                self.full.append(k)


class Moments:
    @staticmethod
    def sems(sizes, pieces, halves):
        n_dp, nf, nm = sizes
        nfm = nf * nm
        dma = pltpu.SemaphoreType.DMA
        return [
            dma((pieces, nfm, halves)),
            dma((pieces, nfm, halves)),
            dma((pieces, n_dp)),
            dma((pieces, n_dp)),
        ]

    def __init__(self, at, moments, first, res, land, sent, got, sems):
        self.at, self.moments, self.first, self.res = at, moments, first, res
        self.land, self.sent, self.got = land, sent, got
        self.as_, self.ar, self.bs, self.br = sems
        self.matrices = moments[0].shape[0]
        self.nfm, self.halves = land[0].shape[:2]
        self.pair = sent.shape[3]

    def part(self, k, f, h):
        at = pl.ds(pl.multiple_of((f * self.halves + h) * LANES, LANES), LANES)
        piece = self.first + k
        return self.moments[piece // self.matrices].at[piece % self.matrices, :, at]

    def local(self, k, f, h):
        return pltpu.make_async_copy(self.part(k, f, h), self.land[k].at[f, h], self.ar.at[k, f, h])

    def start(self, k, j):
        at = self.at
        f = (at.f + j) % self.nfm
        for h in range(self.halves):
            if j == 0:
                self.local(k, f, h).start()
            else:
                remote(
                    self.part(k, f, h), self.land[k].at[at.f, h], self.as_.at[k, f, h], self.ar.at[k, at.f, h], at.fm_device(f)
                ).start()

    def pick(self, k):
        at = self.at
        for j in range(1, self.nfm):
            f = (at.f + self.nfm - j) % self.nfm
            for h in range(self.halves):
                dst = self.land[k].at[f, h]
                remote(dst, dst, self.as_.at[k, f, h], self.ar.at[k, f, h], at.fm_device(f)).wait_recv()
        for h in range(self.halves):
            self.local(k, at.f, h).wait()

        def rows_of(f, carry):
            for i in range(at.n_dp):
                for h in range(self.halves):
                    rows = self.land[k][f, h, pl.ds(self.res[i], self.pair, stride=at.n_dp), :]
                    self.sent[k, i, f, :, h * LANES : (h + 1) * LANES] = rows
            return carry

        lax.fori_loop(0, self.nfm, rows_of, 0)

    def target(self, k, d):
        return self.got.at[k, pl.ds(d * self.nfm, self.nfm)]

    def own(self, k):
        return pltpu.make_async_copy(self.sent.at[k, self.at.d], self.target(k, self.at.d), self.br.at[k, self.at.d])

    def send(self, k):
        at = self.at
        for j in range(1, at.n_dp):
            i = (at.d + j) % at.n_dp
            remote(
                self.sent.at[k, i], self.target(k, at.d), self.bs.at[k, i], self.br.at[k, at.d], (i, at.z, at.y)
            ).start()
        self.own(k).start()

    def finish(self, k):
        at = self.at
        for j in range(1, at.n_dp):
            i = (at.d + at.n_dp - j) % at.n_dp
            dst = self.target(k, i)
            remote(dst, dst, self.bs.at[k, i], self.br.at[k, i], (i, at.z, at.y)).wait_recv()
        self.own(k).wait()
        for j in range(1, at.n_dp):
            i = (at.d + j) % at.n_dp
            remote(
                self.sent.at[k, i], self.target(k, at.d), self.bs.at[k, i], self.br.at[k, at.d], (i, at.z, at.y)
            ).wait_send()
        for j in range(1, self.nfm):
            f = (at.f + j) % self.nfm
            for h in range(self.halves):
                src = self.part(k, f, h)
                remote(src, src, self.as_.at[k, f, h], self.ar.at[k, f, h], at.fm_device(f)).wait_send()


def moment_scratch(sizes, pieces, rows, columns):
    n_dp, nf, nm = sizes
    nfm = nf * nm
    group = columns // nfm
    halves = group // LANES
    return (
        [pltpu.VMEM((nfm, halves, rows, LANES), jnp.float32)] * pieces
        + [pltpu.VMEM((pieces, n_dp, nfm, rows // n_dp, group), jnp.float32)]
        + Moments.sems(sizes, pieces, halves)
    )


class Turns:
    def __init__(self, moments, drip, pieces):
        self.moments, self.drip, self.pieces = moments, drip, pieces
        self.picked = []

    def some(self, count=1):
        picked = self.picked
        for _ in range(count):
            if self.drip.full:
                k = self.drip.full.pop(0)
                self.moments.pick(k)
                picked.append(k)
                if len(picked) > 1:
                    self.moments.send(picked[-2])
            elif picked and picked[-1] != self.pieces and not self.drip.left:
                self.moments.send(picked[-1])
                picked.append(self.pieces)

    def finish(self):
        for k in range(self.pieces):
            self.moments.finish(k)


class Residues:
    @staticmethod
    def scratch(sizes):
        n_dp = sizes[0]
        dma = pltpu.SemaphoreType.DMA
        return [pltpu.VMEM((n_dp, 8, LANES), jnp.int32), pltpu.SMEM((n_dp, 8, LANES), jnp.int32)] + [
            dma((n_dp,)),
            dma((n_dp,)),
            dma((1,)),
        ]

    def __init__(self, at, own, refs):
        self.at, self.own = at, own
        self.held, self.table, self.ss, self.rs, self.ls = refs

    def __getitem__(self, i):
        return self.table[i, 2, 1]

    def begin(self):
        at = self.at
        for j in range(1, at.n_dp):
            i = (at.d + j) % at.n_dp
            remote(self.own, self.held.at[at.d], self.ss.at[i], self.rs.at[at.d], (i, at.z, at.y)).start()
        pltpu.make_async_copy(self.own, self.held.at[at.d], self.rs.at[at.d]).start()

    def finish(self):
        at = self.at
        for j in range(1, at.n_dp):
            i = (at.d + at.n_dp - j) % at.n_dp
            dst = self.held.at[i]
            remote(dst, dst, self.ss.at[i], self.rs.at[i], (i, at.z, at.y)).wait_recv()
            i = (at.d + j) % at.n_dp
            remote(self.own, dst, self.ss.at[i], self.rs.at[i], (i, at.z, at.y)).wait_send()
        pltpu.make_async_copy(self.own, self.held.at[at.d], self.rs.at[at.d]).wait()
        copy = pltpu.make_async_copy(self.held, self.table, self.ls.at[0])
        copy.start()
        copy.wait()


def inputs_kernel(sizes, early_count, tok_ref, w_ref, first_ref, second_ref, res_ref, *refs):
    if early_count:
        (xall_ref, wall_ref, got_ref, tab_ref), refs = refs[:4], refs[4:]
    else:
        (xall_ref, wall_ref), refs = refs[:2], refs[2:]
    as_sem, ar_sem, wl_sem, *sems = refs
    at = Where(sizes)
    group = wall_ref.shape[3]
    planes, sems = plane_chunks(at, tok_ref, xall_ref, sems, tok_ref.shape[0] // IN_CHUNKS)
    along = DpSpread(at, wall_ref, sems[:4])
    moments = residues = tabs = None
    if early_count:
        sems = sems[4:]
        step = len(PlaneSpread.sems(sizes))
        beside = DpSpread(at, tab_ref, sems[step : step + 4])
        tabs = PlaneSpread(at, res_ref, tab_ref, sems[:step], at.d * at.nfm, beside.send)
        sems = sems[step + 4 :]
        residues = Residues(at, res_ref, sems[:5])
        land, sent, sems = sems[5 : 5 + early_count], sems[5 + early_count], sems[6 + early_count :]
        moments = Moments(at, (first_ref, second_ref), 0, residues, land, sent, got_ref, sems)
    drip = Drip(moments.start if moments else None, range(early_count), at.nfm)
    turns = Turns(moments, drip, early_count)
    at.greet(diagonal=early_count > 0)
    if residues:
        residues.begin()
        tabs.begin()
    mine = wall_ref.at[at.d * at.nfm + at.f]

    def columns(f):
        return w_ref.at[0:3, :, pl.ds(pl.multiple_of(f * group, group), group)]

    for j in range(1, at.nfm):
        f = (at.f + j) % at.nfm
        remote(columns(f), mine, as_sem.at[j - 1], ar_sem.at[j - 1], at.fm_device(f)).start()
    for plane in planes:
        plane.begin()
    local = pltpu.make_async_copy(columns(at.f), mine, wl_sem.at[0])
    local.start()
    along.send(at.f, columns(at.f))
    for j in range(1, at.nfm):
        f = (at.f + at.nfm - j) % at.nfm
        dst = wall_ref.at[at.d * at.nfm + f]
        remote(dst, dst, as_sem.at[j - 1], ar_sem.at[j - 1], at.fm_device(f)).wait_recv()
        along.send(f, dst)
    for s in range(1, at.nf):
        if tabs:
            tabs.step(s)
        for plane in planes:
            plane.step(s)
            drip.some(EARLY_STEPS)
        if s == 1:
            for j in range(at.nfm):
                along.forward((at.f + at.nfm - j) % at.nfm)
    for s in range(at.nf):
        if tabs:
            tabs.sides(s)
        for plane in planes:
            plane.sides(s)
            drip.some(EARLY_SIDES)
        if s == 0:
            if residues:
                residues.finish()
        else:
            turns.some(1)
    drip.some(len(drip.left))
    turns.some(early_count)
    turns.some(1)
    if tabs:
        for f in range(at.nfm):
            beside.forward((at.f + f) % at.nfm)
        beside.landed()
        beside.finish()
        tabs.finish()
    along.landed()
    along.finish()
    for plane in planes:
        plane.finish()
    local.wait()
    turns.finish()
    for j in range(1, at.nfm):
        remote(mine, mine, as_sem.at[j - 1], ar_sem.at[j - 1], at.fm_device(at.f)).wait_send()


def share_inputs(sizes, tokens_in, old_weights, old_first, old_second, tables, early_count=0):
    n_dp, nf, nm = sizes
    nfm = nf * nm
    rows, columns = old_weights.shape[1:]
    dma = pltpu.SemaphoreType.DMA
    return pl.pallas_call(
        functools.partial(inputs_kernel, sizes, early_count),
        out_shape=(
            jax.ShapeDtypeStruct((nfm,) + tokens_in.shape, tokens_in.dtype),
            jax.ShapeDtypeStruct((n_dp * nfm, 3, rows, columns // nfm), old_weights.dtype),
        )
        + ((jax.ShapeDtypeStruct((early_count, n_dp * nfm, rows // n_dp, columns // nfm), old_first.dtype),) if early_count else ())
        + ((jax.ShapeDtypeStruct((n_dp * nfm,) + tables.shape, tables.dtype),) if early_count else ()),
        in_specs=[ANY, ANY, ANY, ANY, ANY],
        out_specs=(ANY, ANY, ANY, ANY) if early_count else (ANY, ANY),
        scratch_shapes=[dma((nfm - 1,)), dma((nfm - 1,)), dma((1,))]
        + PlaneSpread.sems(sizes) * IN_CHUNKS
        + DpSpread.sems(sizes)
        + (PlaneSpread.sems(sizes) + DpSpread.sems(sizes) if early_count else [])
        + (Residues.scratch(sizes) + moment_scratch(sizes, early_count, rows, columns) if early_count else []),
        compiler_params=pltpu.CompilerParams(collective_id=0, has_side_effects=True),
        name="share_inputs",
    )(tokens_in, old_weights, old_first, old_second, tables)


def outputs_kernel(sizes, att_ref, w_ref, aall_ref, oall_ref, *sems):
    at = Where(sizes)
    plane = PlaneSpread(at, att_ref, aall_ref, sems[:6])
    along = DpSpread(at, oall_ref, sems[12:16])
    wide = PlaneSpread(at, w_ref.at[3], oall_ref, sems[6:12], at.d * at.nfm, along.send)
    at.greet()
    plane.begin()
    wide.begin()
    for s in range(1, at.nf):
        plane.step(s)
        wide.step(s)
    for s in range(at.nf):
        plane.sides(s)
        wide.sides(s)
    for f in range(at.nfm):
        along.forward((at.f + f) % at.nfm)
    along.landed()
    along.finish()
    plane.finish()
    wide.finish()


def share_outputs(sizes, attended, old_weights):
    n_dp, nf, nm = sizes
    nfm = nf * nm
    rows, columns = old_weights.shape[1:]
    return pl.pallas_call(
        functools.partial(outputs_kernel, sizes),
        out_shape=(
            jax.ShapeDtypeStruct((nfm,) + attended.shape, attended.dtype),
            jax.ShapeDtypeStruct((n_dp * nfm, rows, columns), old_weights.dtype),
        ),
        in_specs=[ANY, ANY],
        out_specs=(ANY, ANY),
        scratch_shapes=PlaneSpread.sems(sizes) + PlaneSpread.sems(sizes) + DpSpread.sems(sizes),
        compiler_params=pltpu.CompilerParams(collective_id=1, has_side_effects=True),
        name="share_outputs",
    )(attended, old_weights)


def keep_residue(full, wide_ref, chosen_ref, res, dp_count):
    rows = wide_ref.shape[1] // dp_count
    for c in range(wide_ref.shape[0]):
        at = slice(c * LANES, (c + 1) * LANES)
        wide_ref[c] = full[:, at].astype(jnp.float32)
        chosen_ref[:, at] = wide_ref[c, pl.ds(res, rows, stride=dp_count), :].astype(chosen_ref.dtype)


def attend_kernel(
    dp_count, place_ref, res_ref, x_ref, wall_ref, segr_ref, segc_ref, att_ref, kept_ref, wbuf, wide, q_ref, k_ref, v_ref, sems
):
    blocks, _, rows, _ = wall_ref.shape
    seq, group = att_ref.shape

    def fetch(p):
        at = pl.ds(pl.multiple_of(place_ref[p] * rows, rows), rows)
        return pltpu.make_async_copy(wall_ref.at[p], wbuf.at[:, at], sems.at[p])

    for p in range(blocks):
        fetch(p).start()
    for p in range(blocks):
        fetch(p).wait()
    tile = 256

    def project(i, carry):
        at = pl.ds(pl.multiple_of(i * tile, tile), tile)
        x = x_ref[at, :]
        for m, ref in enumerate((q_ref, k_ref, v_ref)):
            ref[at, :] = jnp.dot(x, wbuf[m], preferred_element_type=jnp.float32).astype(jnp.bfloat16)
        return carry

    lax.fori_loop(0, seq // tile, project, 0)
    scale = 1.0 / math.sqrt(HD)
    for i in range(seq // tile):
        low, high = i * tile, (i + 1) * tile
        rowid = lax.broadcasted_iota(jnp.int32, (tile, high), 0) + low
        colid = lax.broadcasted_iota(jnp.int32, (tile, high), 1)
        allowed = (rowid >= colid) & (segc_ref[low:high, :1] == segr_ref[:1, :high])
        for h in range(group // HD):
            cols = slice(h * HD, (h + 1) * HD)
            scores = lax.dot_general(
                q_ref[low:high, cols], k_ref[:high, cols], (((1,), (1,)), ((), ())), preferred_element_type=jnp.float32
            )
            scores = jnp.where(allowed, scores * scale, -1e30)
            expo = jnp.exp(scores - jnp.max(scores, axis=1, keepdims=True))
            soft = (expo / jnp.sum(expo, axis=1, keepdims=True)).astype(jnp.bfloat16)
            out = jnp.dot(soft, v_ref[:high, cols], preferred_element_type=jnp.float32)
            att_ref[low:high, cols] = out.astype(jnp.bfloat16)
    for m in range(3):
        keep_residue(wbuf.at[m], wide, kept_ref.at[m], res_ref[0], dp_count)


def attend(dp_count, place, own_res, x_full, wall, segments):
    seq, width = x_full.shape
    blocks, _, rows, group = wall.shape
    bf16, f32 = jnp.bfloat16, jnp.float32
    return pl.pallas_call(
        functools.partial(attend_kernel, dp_count),
        out_shape=(
            jax.ShapeDtypeStruct((seq, group), bf16),
            jax.ShapeDtypeStruct((3, width // dp_count, group), bf16),
        ),
        in_specs=[SMEM, SMEM, VMEM, ANY, VMEM, VMEM],
        out_specs=(VMEM, VMEM),
        scratch_shapes=[
            pltpu.VMEM((3, width, group), bf16),
            pltpu.VMEM((group // LANES, width, LANES), f32),
            pltpu.VMEM((seq, group), bf16),
            pltpu.VMEM((seq, group), bf16),
            pltpu.VMEM((seq, group), bf16),
            pltpu.SemaphoreType.DMA((blocks,)),
        ],
        compiler_params=pltpu.CompilerParams(vmem_limit_bytes=VMEM_MOST),
        cost_estimate=pl.CostEstimate(flops=8 * 10**9, bytes_accessed=3 * 10**7, transcendentals=10**6),
        name="attend",
    )(place, own_res, x_full, wall, segments[None, :], segments[:, None])


def head_kernel(
    dp_count, place_ref, res_ref, f_ref, x_ref, a_ref, oall_ref, hw_ref, gain_ref, tgt_ref, out_ref, kept_ref,
    obuf, hbuf, wide, abuf, hid, norm, sems, hsem,
):
    blocks, rows, columns = oall_ref.shape
    tile, width = x_ref.shape
    fm_count, _, group = a_ref.shape
    vocab = hw_ref.shape[1]
    chunk = 256

    def fetch(p):
        at = pl.ds(pl.multiple_of(place_ref[p] * rows, rows), rows)
        return pltpu.make_async_copy(oall_ref.at[p], obuf.at[at], sems.at[p])

    def fetch_head():
        return pltpu.make_async_copy(hw_ref, hbuf, hsem.at[0])

    @pl.when(pl.program_id(0) == 0)
    def _():
        for p in range(blocks):
            fetch(p).start()
        fetch_head().start()
        for p in range(blocks):
            fetch(p).wait()

    for f in range(fm_count):
        abuf[:, f * group : (f + 1) * group] = a_ref[f]

    def hidden(i, total):
        at = pl.ds(pl.multiple_of(i * chunk, chunk), chunk)
        part = lax.dot_general(
            abuf[...], obuf[at, :], (((1,), (1,)), ((), ())), preferred_element_type=jnp.float32
        )
        part = part + x_ref[:, at].astype(jnp.float32)
        hid[:, at] = part
        return total + jnp.sum(part * part, axis=1, keepdims=True)

    total = lax.fori_loop(0, width // chunk, hidden, jnp.zeros((tile, 1), jnp.float32))
    scale = lax.rsqrt(total / width + 1e-05)

    def normed(i, carry):
        at = pl.ds(pl.multiple_of(i * chunk, chunk), chunk)
        norm[:, at] = (hid[:, at] * scale * gain_ref[:, at]).astype(jnp.bfloat16)
        return carry

    lax.fori_loop(0, width // chunk, normed, 0)

    @pl.when(pl.program_id(0) == 0)
    def _():
        fetch_head().wait()
        own = pl.ds(pl.multiple_of(f_ref[0] * group, group), group)
        keep_residue(obuf[:, own], wide, kept_ref, res_ref[0], dp_count)

    local = tgt_ref[:, :1] - f_ref[0] * vocab
    lane = lax.broadcasted_iota(jnp.int32, (tile, chunk), 1)

    def score(i, carry):
        top, total, picked = carry
        at = pl.ds(pl.multiple_of(i * chunk, chunk), chunk)
        logits = jnp.dot(norm[...], hbuf[:, at], preferred_element_type=jnp.float32)
        higher = jnp.maximum(top, jnp.max(logits, axis=1, keepdims=True))
        total = total * jnp.exp(top - higher) + jnp.sum(jnp.exp(logits - higher), axis=1, keepdims=True)
        hit = jnp.where(lane + i * chunk == local, logits, 0.0)
        return higher, total, picked + jnp.sum(hit, axis=1, keepdims=True)

    zero = jnp.zeros((tile, 1), jnp.float32)
    top, total, picked = lax.fori_loop(0, vocab // chunk, score, (zero - 1e30, zero, zero))
    lanes = lax.broadcasted_iota(jnp.int32, (tile, 128), 1)
    out_ref[...] = jnp.where(lanes == 0, top, jnp.where(lanes == 1, total, picked))


def head_parts(dp_count, place, own_res, own_f, x_full, a_all, oall, head_weight, norm_gain, targets):
    seq, width = x_full.shape
    fm_count, _, group = a_all.shape
    blocks, rows, columns = oall.shape
    vocab = head_weight.shape[1]
    tile = 256
    bf16, f32 = jnp.bfloat16, jnp.float32
    return pl.pallas_call(
        functools.partial(head_kernel, dp_count),
        grid=(seq // tile,),
        out_shape=(
            jax.ShapeDtypeStruct((seq, 128), f32),
            jax.ShapeDtypeStruct((width // dp_count, group), bf16),
        ),
        in_specs=[
            SMEM,
            SMEM,
            SMEM,
            pl.BlockSpec((tile, width), lambda i: (i, 0)),
            pl.BlockSpec((fm_count, tile, group), lambda i: (0, i, 0)),
            ANY,
            ANY,
            pl.BlockSpec((1, width), lambda i: (0, 0)),
            pl.BlockSpec((tile, 1), lambda i: (i, 0)),
        ],
        out_specs=(
            pl.BlockSpec((tile, 128), lambda i: (i, 0)),
            pl.BlockSpec((width // dp_count, group), lambda i: (0, 0)),
        ),
        scratch_shapes=[
            pltpu.VMEM((width, columns), bf16),
            pltpu.VMEM((width, vocab), bf16),
            pltpu.VMEM((group // LANES, width, LANES), f32),
            pltpu.VMEM((tile, columns), bf16),
            pltpu.VMEM((tile, width), f32),
            pltpu.VMEM((tile, width), bf16),
            pltpu.SemaphoreType.DMA((blocks,)),
            pltpu.SemaphoreType.DMA((1,)),
        ],
        compiler_params=pltpu.CompilerParams(vmem_limit_bytes=VMEM_MOST),
        cost_estimate=pl.CostEstimate(flops=2 * 10**10, bytes_accessed=4 * 10**7, transcendentals=10**6),
        name="head_parts",
    )(place, own_res, own_f, x_full, a_all, oall, head_weight, norm_gain[None, :], targets[:, None])


def in_blocks(wall, table, holder):
    if wall.shape[-2] % 16 == 0:
        return wall, table
    ordered = jnp.take(wall, holder, axis=0, mode="clip")
    blocks, rows = ordered.shape[0], ordered.shape[-2]
    join = 16 // math.gcd(16, rows)
    middle = ordered.shape[1:-2]
    ordered = ordered.reshape((blocks // join, join) + middle + ordered.shape[-2:])
    ordered = jnp.moveaxis(ordered, 1, -3)
    ordered = ordered.reshape((blocks // join,) + middle + (join * rows, ordered.shape[-1]))
    return ordered, jnp.arange(blocks // join, dtype=jnp.int32)


def body(
    sizes,
    tokens_in,
    segment_ids,
    target_ids,
    old_weights,
    old_first,
    old_second,
    old_block,
    new_residue,
    norm_gain,
    head_weight,
):
    dp_count, nf, nm = sizes
    fm_count = nf * nm
    segments, targets, table, residues = share_tables(segment_ids, target_ids, old_block, new_residue)
    holder = inverse_of(table)
    own_f = lax.axis_index(("fsdp", "mp"))[None]
    first_sent = pack_moments(old_first, residues, fm_count)
    second_sent = pack_moments(old_second, residues, fm_count)
    first_got = lax.all_to_all(first_sent, EVERYONE, split_axis=0, concat_axis=0, tiled=True)
    second_got = lax.all_to_all(second_sent, EVERYONE, split_axis=0, concat_axis=0, tiled=True)
    x_all, wall = share_inputs(sizes, tokens_in, old_weights, old_first, old_second, table)
    x_full = x_all.reshape(-1, tokens_in.shape[1])
    wall, place = in_blocks(wall, table, holder)
    attended, kept = attend(dp_count, place, new_residue, x_full, wall, segments)
    a_all, oall = share_outputs(sizes, attended, old_weights)
    oall, place = in_blocks(oall, table, holder)
    parts, kept_out = head_parts(
        dp_count, place, new_residue, own_f, x_full, a_all, oall, head_weight, norm_gain, targets
    )
    loss = joint_loss(parts[:, :3].T)
    new_weights = jnp.concatenate([kept, kept_out[None]])
    new_first = unpack_moments(first_got, table, holder)
    new_second = unpack_moments(second_got, table, holder)
    return (new_weights, new_first, new_second, loss)


def final_kernel(
    sizes, early_count, holder_ref, res_ref, att_ref, w_ref, first_ref, second_ref, x_ref, hw_ref, gain_ref,
    tgt_ref, out_ref, kept_ref, got_ref, owall, obuf, xbuf, hbuf, abuf, hid, norm, wide, wsem, *sems,
):
    at = Where(sizes)
    blocks, rows, columns = owall.shape
    seq, width = xbuf.shape
    _, _, group = abuf.shape
    vocab = hbuf.shape[1]
    tiles = seq // ROW_TILE
    chunk = 256
    pieces = got_ref.shape[0]
    step = len(PlaneSpread.sems(sizes))
    planes, sems = plane_chunks(at, att_ref, abuf, sems, ROW_TILE)
    along = DpSpread(at, owall, sems[step : step + 4])
    whole = PlaneSpread(at, w_ref.at[3], owall, sems[:step], at.d * at.nfm, along.send)
    sems = sems[step + 4 :]
    land, sent, sems = sems[:pieces], sems[pieces], sems[pieces + 1 :]
    moments = Moments(at, (first_ref, second_ref), early_count, res_ref, land, sent, got_ref, sems)
    loads = [pltpu.make_async_copy(x_ref, xbuf, wsem.at[0]), pltpu.make_async_copy(hw_ref, hbuf, wsem.at[1])]
    at.greet(diagonal=True)
    whole.begin()
    for plane in planes:
        plane.begin()
    for load in loads:
        load.start()
    drip = Drip(moments.start, range(pieces), at.nfm)
    turns = Turns(moments, drip, pieces)
    for s in range(1, at.nf):
        for plane in [whole] + planes:
            plane.step(s)
            drip.some(LATE_STEPS)
    for s in range(at.nf):
        for plane in [whole] + planes:
            plane.sides(s)
            drip.some(LATE_SIDES)
        if s >= TURN_FROM:
            turns.some(1)
    drip.some(len(drip.left))
    turns.some(TURNS)
    for f in range(at.nfm):
        along.forward((at.f + f) % at.nfm)
    turns.some(TURNS_AFTER)
    along.landed()
    own = whole.slot(at.z, at.y)
    pltpu.make_async_copy(whole.own, own, whole.lc.at[0]).wait()

    def order(b, carry):
        obuf[pl.ds(pl.multiple_of(b * rows, rows), rows), :] = owall[holder_ref[b]]
        return carry

    lax.fori_loop(0, blocks, order, 0)
    for load in loads:
        load.wait()
    for plane in planes:
        pltpu.make_async_copy(plane.own, plane.slot(at.z, at.y), plane.lc.at[0]).wait()
    lane = lax.broadcasted_iota(jnp.int32, (ROW_TILE, chunk), 1)
    lanes = lax.broadcasted_iota(jnp.int32, (ROW_TILE, LANES), 1)

    def one_tile(t, carry):
        here = pl.ds(pl.multiple_of(t * ROW_TILE, ROW_TILE), ROW_TILE)

        def hidden(i, total):
            cols = pl.ds(pl.multiple_of(i * chunk, chunk), chunk)
            part = xbuf[here, cols].astype(jnp.float32)
            for f in range(at.nfm):
                part += lax.dot_general(
                    abuf[f, here, :],
                    obuf[cols, f * group : (f + 1) * group],
                    (((1,), (1,)), ((), ())),
                    preferred_element_type=jnp.float32,
                )
            hid[:, cols] = part
            return total + jnp.sum(part * part, axis=1, keepdims=True)

        total = lax.fori_loop(0, width // chunk, hidden, jnp.zeros((ROW_TILE, 1), jnp.float32))
        scale = lax.rsqrt(total / width + 1e-05)

        def normed(i, carry):
            cols = pl.ds(pl.multiple_of(i * chunk, chunk), chunk)
            norm[:, cols] = (hid[:, cols] * scale * gain_ref[:, cols]).astype(jnp.bfloat16)
            return carry

        lax.fori_loop(0, width // chunk, normed, 0)
        local = tgt_ref[here, :1] - at.f * vocab

        def score(i, carry):
            top, total, picked = carry
            cols = pl.ds(pl.multiple_of(i * chunk, chunk), chunk)
            logits = jnp.dot(norm[...], hbuf[:, cols], preferred_element_type=jnp.float32)
            higher = jnp.maximum(top, jnp.max(logits, axis=1, keepdims=True))
            total = total * jnp.exp(top - higher) + jnp.sum(jnp.exp(logits - higher), axis=1, keepdims=True)
            hit = jnp.where(lane + i * chunk == local, logits, 0.0)
            return higher, total, picked + jnp.sum(hit, axis=1, keepdims=True)

        zero = jnp.zeros((ROW_TILE, 1), jnp.float32)
        top, total, picked = lax.fori_loop(0, vocab // chunk, score, (zero - 1e30, zero, zero))
        out_ref[here, :] = jnp.where(lanes == 0, top, jnp.where(lanes == 1, total, picked))
        return carry

    for t in range(tiles):
        lax.fori_loop(t, t + 1, one_tile, 0)
        turns.some(1)
    part_rows = wide.shape[0]
    for c in range(group // LANES):
        cols = pl.ds(pl.multiple_of(at.f * group + c * LANES, LANES), LANES)
        for i in range(width // part_rows):
            wide[...] = obuf[i * part_rows : (i + 1) * part_rows, cols].astype(jnp.float32)
            kept = wide[pl.ds(res_ref[at.d], part_rows // at.n_dp, stride=at.n_dp), :]
            kept_rows = part_rows // at.n_dp
            kept_ref[i * kept_rows : (i + 1) * kept_rows, c * LANES : (c + 1) * LANES] = kept.astype(kept_ref.dtype)
    turns.some(pieces)
    turns.some(1)
    along.finish()
    for plane in planes + [whole]:
        plane.sent()
    turns.finish()


def finish_all(sizes, early_count, holder, residues, attended, old_weights, old_first, old_second, x_full,
               head_weight, norm_gain, targets):
    n_dp, nf, nm = sizes
    nfm = nf * nm
    matrices, rows, columns = old_weights.shape
    seq, width = x_full.shape
    vocab = head_weight.shape[1]
    group, devices, pair_rows = columns // nfm, n_dp * nfm, rows // n_dp
    pieces = 2 * matrices - early_count
    bf16, f32 = jnp.bfloat16, jnp.float32
    plane_sems = PlaneSpread.sems(sizes)
    return pl.pallas_call(
        functools.partial(final_kernel, sizes, early_count),
        out_shape=(
            jax.ShapeDtypeStruct((seq, LANES), f32),
            jax.ShapeDtypeStruct((width // n_dp, group), bf16),
            jax.ShapeDtypeStruct((pieces, devices, pair_rows, group), f32),
        ),
        in_specs=[SMEM, SMEM] + [ANY] * 6 + [VMEM, VMEM],
        out_specs=(VMEM, VMEM, ANY),
        scratch_shapes=[
            pltpu.VMEM((devices, rows, columns), bf16),
            pltpu.VMEM((width, columns), bf16),
            pltpu.VMEM((seq, width), bf16),
            pltpu.VMEM((width, vocab), bf16),
            pltpu.VMEM((nfm, seq, group), bf16),
            pltpu.VMEM((ROW_TILE, width), f32),
            pltpu.VMEM((ROW_TILE, width), bf16),
            pltpu.VMEM((width // 4, LANES), f32),
            pltpu.SemaphoreType.DMA((2,)),
        ]
        + plane_sems * (seq // ROW_TILE + 1)
        + DpSpread.sems(sizes)
        + moment_scratch(sizes, pieces, rows, columns),
        compiler_params=pltpu.CompilerParams(
            collective_id=2, has_side_effects=True, vmem_limit_bytes=63 * 1024 * 1024
        ),
        cost_estimate=pl.CostEstimate(flops=2 * 10**10, bytes_accessed=4 * 10**7, transcendentals=10**6),
        name="finish_all",
    )(holder, residues, attended, old_weights, old_first, old_second, x_full, head_weight, norm_gain[None, :],
      targets[:, None])


def body_close(
    sizes,
    tokens_in,
    segment_ids,
    target_ids,
    old_weights,
    old_first,
    old_second,
    old_block,
    new_residue,
    norm_gain,
    head_weight,
):
    dp_count = sizes[0]
    fm_count = sizes[1] * sizes[2]
    scalars = jnp.pad(jnp.concatenate([old_block, new_residue]), (0, LANES - 2))
    own = jnp.pad(jnp.stack([segment_ids, target_ids, scalars]), ((0, 5), (0, 0)))
    x_all, wall, got_early, tables = share_inputs(sizes, tokens_in, old_weights, old_first, old_second, own, EARLY)
    here = lax.dynamic_slice_in_dim(tables, lax.axis_index("dp") * fm_count, fm_count)
    segments, targets = here[:, 0].reshape(-1), here[:, 1].reshape(-1)
    table, residues = tables[:, 2, 0], tables[::fm_count, 2, 1]
    holder = inverse_of(table)
    x_full = x_all.reshape(-1, tokens_in.shape[1])
    attended, kept = attend(dp_count, table, new_residue, x_full, wall, segments)
    parts, kept_out, got = finish_all(
        sizes, EARLY, holder, residues, attended, old_weights, old_first, old_second, x_full, head_weight,
        norm_gain, targets,
    )
    loss = joint_loss(parts[:, :3].T)
    new_weights, new_first, new_second = unpack_all(table, got_early, got, kept, kept_out)
    return (new_weights, new_first, new_second, loss)


def solution(mesh):
    placed = (
        P(EVERYONE, None),
        P(EVERYONE),
        P(EVERYONE),
        P(None, EVERYONE, None),
        P(None, EVERYONE, None),
        P(None, EVERYONE, None),
        P(EVERYONE),
        P("dp"),
        P(),
        P(None, ("fsdp", "mp")),
    )
    sizes = tuple(mesh.shape[name] for name in EVERYONE)

    def step(*args):
        rows, columns = args[3].shape[1:]
        seq = args[0].shape[0] * sizes[1] * sizes[2]
        close = rows % 16 == 0 and (rows // sizes[0]) % 8 == 0 and seq <= 1024 and columns <= 2048
        close = close and args[1].shape[0] == LANES
        return (body_close if close else body)(sizes, *args)

    return jax.shard_map(
        step,
        mesh=mesh,
        in_specs=placed,
        out_specs=(
            P(None, "dp", ("fsdp", "mp")),
            P(None, "dp", ("fsdp", "mp")),
            P(None, "dp", ("fsdp", "mp")),
            P(EVERYONE),
        ),
        check_vma=False,
    )
```

```python
import functools
import math

import jax
import jax.numpy as jnp
from jax import lax
from jax.experimental import pallas as pl
from jax.experimental.pallas import tpu as pltpu
from jax.sharding import PartitionSpec as P

HD = 128
LANES = 128
MESH = pl.DeviceIdType.MESH
ANY = pl.BlockSpec(memory_space=pl.ANY)
SMEM = pl.BlockSpec(memory_space=pltpu.SMEM)
VMEM = pl.BlockSpec(memory_space=pltpu.VMEM)
EVERYONE = ("dp", "fsdp", "mp")
VMEM_MOST = 60 * 1024 * 1024
CORES = 2
EARLY = 2
EARLY_STEPS = 2
EARLY_SIDES = 1
LATE_STEPS = 1
LATE_SIDES = 1
TURNS = 0
TURN_FROM = 9
TURNS_AFTER = 3
IN_CHUNKS = 4
ROW_TILE = 256


def inverse_of(table):
    total_count = table.shape[0]
    places = jnp.arange(total_count, dtype=jnp.int32)
    return jnp.sum(jnp.where(table[None, :] == places[:, None], places[None, :], 0), axis=1)


def share_tables(segment_ids, target_ids, old_block, new_residue):
    own = jnp.concatenate([segment_ids, target_ids, old_block, new_residue])
    rows = jnp.broadcast_to(own[None, None], (lax.axis_size(EVERYONE), 1, own.shape[0]))
    rows = lax.all_to_all(rows, EVERYONE, split_axis=0, concat_axis=0, tiled=True)[:, 0]
    count = segment_ids.shape[0]
    fm_count = lax.axis_size(("fsdp", "mp"))
    here = lax.dynamic_slice_in_dim(rows, lax.axis_index("dp") * fm_count, fm_count)
    segments = here[:, :count].reshape(-1)
    targets = here[:, count : 2 * count].reshape(-1)
    return segments, targets, rows[:, 2 * count], rows[::fm_count, 2 * count + 1]


def joint_loss(parts):
    axes = ("fsdp", "mp")
    fm_count = lax.axis_size(axes)
    own_count = parts.shape[1] // fm_count
    parts = parts.reshape(3, fm_count, own_count).transpose(1, 0, 2)
    parts = lax.all_to_all(parts, axes, split_axis=0, concat_axis=0, tiled=True)
    tops, totals, targets = parts[:, 0], parts[:, 1], parts[:, 2]
    joint_max = jnp.max(tops, axis=0)
    joint_total = jnp.sum(totals * jnp.exp(tops - joint_max[None]), axis=0)
    return joint_max + jnp.log(joint_total) - jnp.sum(targets, axis=0)


def pack_kernel(dp_count, fm_count, res_ref, old_ref, sent_ref, lanes):
    rows, columns = old_ref.shape[1:]
    pair_rows, group = rows // dp_count, columns // fm_count
    for c in range(columns // LANES):
        lanes[c] = old_ref[0, :, c * LANES : (c + 1) * LANES]
    for i in range(dp_count):
        for c in range(columns // LANES):
            f, at = divmod(c * LANES, group)
            chosen = lanes[c, pl.ds(res_ref[i], pair_rows, stride=dp_count), :]
            sent_ref[i * fm_count + f, 0, :, at : at + LANES] = chosen


def pack_moments(stored, residues, fm_count):
    matrices, row_count, columns = stored.shape
    dp_count = residues.shape[0]
    pair_rows, group = row_count // dp_count, columns // fm_count
    devices = dp_count * fm_count
    if pair_rows % 8:
        split_rows = stored.reshape(matrices, pair_rows, dp_count, fm_count, group)
        chosen = jnp.take(split_rows, residues, axis=2, mode="clip")
        return chosen.transpose(2, 3, 0, 1, 4).reshape(devices, matrices, pair_rows, group)
    return pl.pallas_call(
        functools.partial(pack_kernel, dp_count, fm_count),
        grid=(matrices,),
        out_shape=jax.ShapeDtypeStruct((devices, matrices, pair_rows, group), stored.dtype),
        in_specs=[SMEM, pl.BlockSpec((1, row_count, columns), lambda m: (m, 0, 0))],
        out_specs=pl.BlockSpec((devices, 1, pair_rows, group), lambda m: (0, m, 0, 0)),
        scratch_shapes=[pltpu.VMEM((columns // LANES, row_count, LANES), stored.dtype)],
        name="pack_moments",
    )(residues, stored)


def unpack_kernel(which, block_ref, got_ref, out_ref, buf, in_sems, out_sems):
    if which is not None:
        got_ref = got_ref.at[which]
    devices, _, pair_rows, _ = got_ref.shape
    for p in range(devices):
        pltpu.make_async_copy(got_ref.at[p], buf.at[p], in_sems.at[p]).start()
    for p in range(devices):
        pltpu.make_async_copy(got_ref.at[p], buf.at[p], in_sems.at[p]).wait()
        place = pl.ds(pl.multiple_of(block_ref[p] * pair_rows, pair_rows), pair_rows)
        pltpu.make_async_copy(buf.at[p], out_ref.at[:, place], out_sems.at[p]).start()
    for p in range(devices):
        place = pl.ds(pl.multiple_of(block_ref[p] * pair_rows, pair_rows), pair_rows)
        pltpu.make_async_copy(buf.at[p], out_ref.at[:, place], out_sems.at[p]).wait()


def unpack_moments(received, table, holder, which=None):
    devices, matrices, pair_rows, group = received.shape[-4:]
    if pair_rows % 8:
        ordered = jnp.take(received, holder, axis=0, mode="clip")
        return ordered.transpose(1, 0, 2, 3).reshape(matrices, devices * pair_rows, group)
    return pl.pallas_call(
        functools.partial(unpack_kernel, which),
        out_shape=jax.ShapeDtypeStruct((matrices, devices * pair_rows, group), received.dtype),
        in_specs=[SMEM, ANY],
        out_specs=ANY,
        scratch_shapes=[
            pltpu.VMEM(received.shape[-4:], received.dtype),
            pltpu.SemaphoreType.DMA((devices,)),
            pltpu.SemaphoreType.DMA((devices,)),
        ],
        name="unpack_moments",
    )(table, received)


def unpack_all_kernel(block_ref, early_ref, late_ref, kept_ref, last_ref, w_ref, first_ref, second_ref, buf, wbuf, isem, osem, wsem):
    pieces, devices, pair_rows, _ = buf.shape
    early, matrices = early_ref.shape[0], pieces // 2
    load = [
        pltpu.make_async_copy(early_ref.at[k] if k < early else late_ref.at[k - early], buf.at[k], isem.at[k])
        for k in range(pieces)
    ]
    three = [
        pltpu.make_async_copy(kept_ref, wbuf.at[0 : matrices - 1], wsem.at[0]),
        pltpu.make_async_copy(last_ref, wbuf.at[matrices - 1], wsem.at[1]),
    ]
    out = pltpu.make_async_copy(wbuf, w_ref, wsem.at[2])
    for copy in load[:matrices] + three + load[matrices:]:
        copy.start()

    def place(q, p):
        rows = pl.ds(pl.multiple_of(block_ref[p] * pair_rows, pair_rows), pair_rows)
        target = (first_ref, second_ref)[q].at[:, rows]
        return pltpu.make_async_copy(buf.at[q * matrices : (q + 1) * matrices, p], target, osem.at[q, p])

    for q in range(2):
        for k in range(q * matrices, (q + 1) * matrices):
            load[k].wait()
        for p in range(devices):
            place(q, p).start()
        if q == 0:
            for copy in three:
                copy.wait()
            out.start()
    for q in range(2):
        for p in range(devices):
            place(q, p).wait()
    out.wait()


def unpack_all(table, early, late, kept, last):
    _, devices, pair_rows, group = early.shape
    matrices = kept.shape[0] + 1
    moment = jax.ShapeDtypeStruct((matrices, devices * pair_rows, group), early.dtype)
    dma = pltpu.SemaphoreType.DMA
    return pl.pallas_call(
        unpack_all_kernel,
        out_shape=(jax.ShapeDtypeStruct((matrices,) + last.shape, last.dtype), moment, moment),
        in_specs=[SMEM, ANY, ANY, ANY, ANY],
        out_specs=(ANY, ANY, ANY),
        scratch_shapes=[
            pltpu.VMEM((2 * matrices,) + early.shape[1:], early.dtype),
            pltpu.VMEM((matrices,) + last.shape, last.dtype),
            dma((2 * matrices,)),
            dma((2, devices)),
            dma((3,)),
        ],
        name="unpack_all",
    )(table, early, late, kept, last)


def remote(src, dst, send_sem, recv_sem, device):
    return pltpu.make_async_remote_copy(
        src_ref=src,
        dst_ref=dst,
        send_sem=send_sem,
        recv_sem=recv_sem,
        device_id=device,
        device_id_type=MESH,
    )


class Where:
    def __init__(self, sizes):
        self.n_dp, self.nf, self.nm = sizes
        self.nx, self.nfm = self.n_dp // CORES, self.nf * self.nm
        self.d, self.z, self.y = (lax.axis_index(name) for name in EVERYONE)
        self.x, self.c = self.d // CORES, self.d % CORES
        self.f = self.z * self.nm + self.y

    def fm_device(self, f):
        return (self.d, f // self.nm, f % self.nm)

    def greet(self, diagonal=False):
        barrier = pltpu.get_barrier_semaphore()
        peers = [self.fm_device((self.f + j) % self.nfm) for j in range(1, self.nfm)]
        for k in range(1, self.nx):
            peers.append((((self.x + k) % self.nx) * CORES + self.c, self.z, self.y))
            if diagonal:
                peers.append((((self.x + k) % self.nx) * CORES + 1 - self.c, self.z, self.y))
        peers.append((self.x * CORES + 1 - self.c, self.z, self.y))
        for peer in peers:
            pl.semaphore_signal(barrier, inc=1, device_id=peer, device_id_type=MESH)
        pl.semaphore_wait(barrier, len(peers))


class PlaneSpread:
    @staticmethod
    def sems(sizes):
        _, nf, nm = sizes
        dma = pltpu.SemaphoreType.DMA
        return [dma((nf,)), dma((nf,)), dma((nf,)), dma((nf, nm - 1)), dma((nf, nm - 1)), dma((1,))]

    def __init__(self, at, own, out, sems, base=0, arrived=None, rows=None):
        self.at, self.own, self.out, self.base, self.rows = at, own, out, base, rows
        self.up, self.dn, self.ch, self.ys, self.yr, self.lc = sems
        self.arrived = arrived

    def slot(self, z, y):
        slot = self.base + z * self.at.nm + y
        return self.out.at[slot] if self.rows is None else self.out.at[slot, self.rows]

    def _pass(self, zb, src, up, down):
        at = self.at
        dst = self.slot(zb, at.y)
        if up:
            pl.when(at.z + 1 < at.nf)(
                lambda: remote(src, dst, self.up.at[zb], self.ch.at[zb], (at.d, at.z + 1, at.y)).start()
            )
        if down:
            pl.when(at.z > 0)(
                lambda: remote(src, dst, self.dn.at[zb], self.ch.at[zb], (at.d, at.z - 1, at.y)).start()
            )
        for j in range(1, at.nm):
            there = (at.d, at.z, (at.y + j) % at.nm)
            remote(src, dst, self.ys.at[zb, j - 1], self.yr.at[zb, j - 1], there).start()
        if self.arrived:
            self.arrived(zb * at.nm + at.y, src)

    def begin(self):
        at = self.at
        self._pass(at.z, self.own, True, True)
        pltpu.make_async_copy(self.own, self.slot(at.z, at.y), self.lc.at[0]).start()

    def step(self, s):
        at = self.at

        def below():
            zb = at.z - s
            dst = self.slot(zb, at.y)
            remote(dst, dst, self.up.at[zb], self.ch.at[zb], (at.d, at.z, at.y)).wait_recv()
            self._pass(zb, dst, True, False)

        def above():
            zb = at.z + s
            dst = self.slot(zb, at.y)
            remote(dst, dst, self.dn.at[zb], self.ch.at[zb], (at.d, at.z, at.y)).wait_recv()
            self._pass(zb, dst, False, True)

        pl.when(at.z - s >= 0)(below)
        pl.when(at.z + s < at.nf)(above)

    def side(self, zb):
        at = self.at
        for j in range(1, at.nm):
            source = (at.y + at.nm - j) % at.nm
            dst = self.slot(zb, source)
            remote(dst, dst, self.ys.at[zb, j - 1], self.yr.at[zb, j - 1], (at.d, at.z, at.y)).wait_recv()
            if self.arrived:
                self.arrived(zb * at.nm + source, dst)

    def sides(self, s):
        at = self.at
        if s == 0:
            self.side(at.z)
        else:
            pl.when(at.z - s >= 0)(lambda: self.side(at.z - s))
            pl.when(at.z + s < at.nf)(lambda: self.side(at.z + s))

    def finish(self):
        own = self.slot(self.at.z, self.at.y)
        pltpu.make_async_copy(self.own, own, self.lc.at[0]).wait()
        self.sent()

    def sent(self):
        at = self.at
        own = self.slot(at.z, at.y)
        here = (at.d, at.z, at.y)
        for t in range(at.nf):
            for j in range(1, at.nm):
                remote(own, own, self.ys.at[t, j - 1], self.yr.at[t, j - 1], here).wait_send()
            pl.when((t <= at.z) & (at.z + 1 < at.nf))(
                lambda: remote(own, own, self.up.at[t], self.ch.at[t], here).wait_send()
            )
            pl.when((t >= at.z) & (at.z > 0))(
                lambda: remote(own, own, self.dn.at[t], self.ch.at[t], here).wait_send()
            )


def plane_chunks(at, own, out, sems, rows):
    step = len(PlaneSpread.sems((1, 1, 2)))
    planes = []
    for low in range(0, own.shape[0], rows):
        here = slice(low, low + rows)
        planes.append(PlaneSpread(at, own.at[here], out, sems[:step], rows=here))
        sems = sems[step:]
    return planes, sems


class DpSpread:
    @staticmethod
    def sems(sizes):
        n_dp, nf, nm = sizes
        nfm, nx = nf * nm, n_dp // CORES
        dma = pltpu.SemaphoreType.DMA
        return [dma((nfm, max(nx - 1, 1))), dma((nfm, max(nx - 1, 1))), dma((nfm, nx)), dma((nfm, nx))]

    def __init__(self, at, out, sems):
        self.at, self.out = at, out
        self.xs, self.xr, self.cs, self.cr = sems

    def slot(self, x, c, f):
        return self.out.at[(x * CORES + c) * self.at.nfm + f]

    def send(self, f, src):
        at = self.at
        dst = self.slot(at.x, at.c, f)
        for k in range(1, at.nx):
            there = (((at.x + k) % at.nx) * CORES + at.c, at.z, at.y)
            remote(src, dst, self.xs.at[f, k - 1], self.xr.at[f, k - 1], there).start()
        there = (at.x * CORES + 1 - at.c, at.z, at.y)
        remote(src, dst, self.cs.at[f, 0], self.cr.at[f, 0], there).start()

    def forward(self, f):
        at = self.at
        here = (at.d, at.z, at.y)
        there = (at.x * CORES + 1 - at.c, at.z, at.y)
        for k in range(1, at.nx):
            dst = self.slot((at.x + at.nx - k) % at.nx, at.c, f)
            remote(dst, dst, self.xs.at[f, k - 1], self.xr.at[f, k - 1], here).wait_recv()
            remote(dst, dst, self.cs.at[f, k], self.cr.at[f, k], there).start()

    def landed(self):
        at = self.at
        here = (at.d, at.z, at.y)
        for f in range(at.nfm):
            for k in range(at.nx):
                dst = self.slot((at.x + at.nx - k) % at.nx, 1 - at.c, f)
                remote(dst, dst, self.cs.at[f, k], self.cr.at[f, k], here).wait_recv()

    def finish(self):
        at = self.at
        here = (at.d, at.z, at.y)
        for f in range(at.nfm):
            for k in range(at.nx):
                dst = self.slot(at.x, at.c, f)
                remote(dst, dst, self.cs.at[f, k], self.cr.at[f, k], here).wait_send()
            for k in range(1, at.nx):
                dst = self.slot(at.x, at.c, f)
                remote(dst, dst, self.xs.at[f, k - 1], self.xr.at[f, k - 1], here).wait_send()


class Drip:
    def __init__(self, start, pieces, count):
        self.start = start
        self.left = [(k, j) for k in pieces for j in range(count)]
        self.full = []
        self.count = count

    def some(self, number):
        for _ in range(min(number, len(self.left))):
            k, j = self.left.pop(0)
            self.start(k, j)
            if j == self.count - 1:
                self.full.append(k)


class Moments:
    @staticmethod
    def sems(sizes, pieces, halves):
        n_dp, nf, nm = sizes
        nfm = nf * nm
        dma = pltpu.SemaphoreType.DMA
        return [
            dma((pieces, nfm, halves)),
            dma((pieces, nfm, halves)),
            dma((pieces, n_dp)),
            dma((pieces, n_dp)),
        ]

    def __init__(self, at, moments, first, res, land, sent, got, sems):
        self.at, self.moments, self.first, self.res = at, moments, first, res
        self.land, self.sent, self.got = land, sent, got
        self.as_, self.ar, self.bs, self.br = sems
        self.matrices = moments[0].shape[0]
        self.nfm, self.halves = land[0].shape[:2]
        self.pair = sent.shape[3]

    def part(self, k, f, h):
        at = pl.ds(pl.multiple_of((f * self.halves + h) * LANES, LANES), LANES)
        piece = self.first + k
        return self.moments[piece // self.matrices].at[piece % self.matrices, :, at]

    def local(self, k, f, h):
        return pltpu.make_async_copy(self.part(k, f, h), self.land[k].at[f, h], self.ar.at[k, f, h])

    def start(self, k, j):
        at = self.at
        f = (at.f + j) % self.nfm
        for h in range(self.halves):
            if j == 0:
                self.local(k, f, h).start()
            else:
                remote(
                    self.part(k, f, h), self.land[k].at[at.f, h], self.as_.at[k, f, h], self.ar.at[k, at.f, h], at.fm_device(f)
                ).start()

    def pick(self, k):
        at = self.at
        for j in range(1, self.nfm):
            f = (at.f + self.nfm - j) % self.nfm
            for h in range(self.halves):
                dst = self.land[k].at[f, h]
                remote(dst, dst, self.as_.at[k, f, h], self.ar.at[k, f, h], at.fm_device(f)).wait_recv()
        for h in range(self.halves):
            self.local(k, at.f, h).wait()

        def rows_of(f, carry):
            for i in range(at.n_dp):
                for h in range(self.halves):
                    rows = self.land[k][f, h, pl.ds(self.res[i], self.pair, stride=at.n_dp), :]
                    self.sent[k, i, f, :, h * LANES : (h + 1) * LANES] = rows
            return carry

        lax.fori_loop(0, self.nfm, rows_of, 0)

    def target(self, k, d):
        return self.got.at[k, pl.ds(d * self.nfm, self.nfm)]

    def own(self, k):
        return pltpu.make_async_copy(self.sent.at[k, self.at.d], self.target(k, self.at.d), self.br.at[k, self.at.d])

    def send(self, k):
        at = self.at
        for j in range(1, at.n_dp):
            i = (at.d + j) % at.n_dp
            remote(
                self.sent.at[k, i], self.target(k, at.d), self.bs.at[k, i], self.br.at[k, at.d], (i, at.z, at.y)
            ).start()
        self.own(k).start()

    def finish(self, k):
        at = self.at
        for j in range(1, at.n_dp):
            i = (at.d + at.n_dp - j) % at.n_dp
            dst = self.target(k, i)
            remote(dst, dst, self.bs.at[k, i], self.br.at[k, i], (i, at.z, at.y)).wait_recv()
        self.own(k).wait()
        for j in range(1, at.n_dp):
            i = (at.d + j) % at.n_dp
            remote(
                self.sent.at[k, i], self.target(k, at.d), self.bs.at[k, i], self.br.at[k, at.d], (i, at.z, at.y)
            ).wait_send()
        for j in range(1, self.nfm):
            f = (at.f + j) % self.nfm
            for h in range(self.halves):
                src = self.part(k, f, h)
                remote(src, src, self.as_.at[k, f, h], self.ar.at[k, f, h], at.fm_device(f)).wait_send()


def moment_scratch(sizes, pieces, rows, columns):
    n_dp, nf, nm = sizes
    nfm = nf * nm
    group = columns // nfm
    halves = group // LANES
    return (
        [pltpu.VMEM((nfm, halves, rows, LANES), jnp.float32)] * pieces
        + [pltpu.VMEM((pieces, n_dp, nfm, rows // n_dp, group), jnp.float32)]
        + Moments.sems(sizes, pieces, halves)
    )


class Turns:
    def __init__(self, moments, drip, pieces):
        self.moments, self.drip, self.pieces = moments, drip, pieces
        self.picked = []

    def some(self, count=1):
        picked = self.picked
        for _ in range(count):
            if self.drip.full:
                k = self.drip.full.pop(0)
                self.moments.pick(k)
                picked.append(k)
                if len(picked) > 1:
                    self.moments.send(picked[-2])
            elif picked and picked[-1] != self.pieces and not self.drip.left:
                self.moments.send(picked[-1])
                picked.append(self.pieces)

    def finish(self):
        for k in range(self.pieces):
            self.moments.finish(k)


class Residues:
    @staticmethod
    def scratch(sizes):
        n_dp = sizes[0]
        dma = pltpu.SemaphoreType.DMA
        return [pltpu.VMEM((n_dp, 8, LANES), jnp.int32), pltpu.SMEM((n_dp, 8, LANES), jnp.int32)] + [
            dma((n_dp,)),
            dma((n_dp,)),
            dma((1,)),
        ]

    def __init__(self, at, own, refs):
        self.at, self.own = at, own
        self.held, self.table, self.ss, self.rs, self.ls = refs

    def __getitem__(self, i):
        return self.table[i, 2, 1]

    def begin(self):
        at = self.at
        for j in range(1, at.n_dp):
            i = (at.d + j) % at.n_dp
            remote(self.own, self.held.at[at.d], self.ss.at[i], self.rs.at[at.d], (i, at.z, at.y)).start()
        pltpu.make_async_copy(self.own, self.held.at[at.d], self.rs.at[at.d]).start()

    def finish(self):
        at = self.at
        for j in range(1, at.n_dp):
            i = (at.d + at.n_dp - j) % at.n_dp
            dst = self.held.at[i]
            remote(dst, dst, self.ss.at[i], self.rs.at[i], (i, at.z, at.y)).wait_recv()
            i = (at.d + j) % at.n_dp
            remote(self.own, dst, self.ss.at[i], self.rs.at[i], (i, at.z, at.y)).wait_send()
        pltpu.make_async_copy(self.own, self.held.at[at.d], self.rs.at[at.d]).wait()
        copy = pltpu.make_async_copy(self.held, self.table, self.ls.at[0])
        copy.start()
        copy.wait()


def inputs_kernel(sizes, early_count, tok_ref, w_ref, first_ref, second_ref, res_ref, *refs):
    if early_count:
        (xall_ref, wall_ref, got_ref, tab_ref), refs = refs[:4], refs[4:]
    else:
        (xall_ref, wall_ref), refs = refs[:2], refs[2:]
    as_sem, ar_sem, wl_sem, *sems = refs
    at = Where(sizes)
    group = wall_ref.shape[3]
    planes, sems = plane_chunks(at, tok_ref, xall_ref, sems, tok_ref.shape[0] // IN_CHUNKS)
    along = DpSpread(at, wall_ref, sems[:4])
    moments = residues = tabs = None
    if early_count:
        sems = sems[4:]
        step = len(PlaneSpread.sems(sizes))
        beside = DpSpread(at, tab_ref, sems[step : step + 4])
        tabs = PlaneSpread(at, res_ref, tab_ref, sems[:step], at.d * at.nfm, beside.send)
        sems = sems[step + 4 :]
        residues = Residues(at, res_ref, sems[:5])
        land, sent, sems = sems[5 : 5 + early_count], sems[5 + early_count], sems[6 + early_count :]
        moments = Moments(at, (first_ref, second_ref), 0, residues, land, sent, got_ref, sems)
    drip = Drip(moments.start if moments else None, range(early_count), at.nfm)
    turns = Turns(moments, drip, early_count)
    at.greet(diagonal=early_count > 0)
    if residues:
        residues.begin()
        tabs.begin()
    mine = wall_ref.at[at.d * at.nfm + at.f]

    def columns(f):
        return w_ref.at[0:3, :, pl.ds(pl.multiple_of(f * group, group), group)]

    for j in range(1, at.nfm):
        f = (at.f + j) % at.nfm
        remote(columns(f), mine, as_sem.at[j - 1], ar_sem.at[j - 1], at.fm_device(f)).start()
    for plane in planes:
        plane.begin()
    local = pltpu.make_async_copy(columns(at.f), mine, wl_sem.at[0])
    local.start()
    along.send(at.f, columns(at.f))
    for j in range(1, at.nfm):
        f = (at.f + at.nfm - j) % at.nfm
        dst = wall_ref.at[at.d * at.nfm + f]
        remote(dst, dst, as_sem.at[j - 1], ar_sem.at[j - 1], at.fm_device(f)).wait_recv()
        along.send(f, dst)
    for s in range(1, at.nf):
        if tabs:
            tabs.step(s)
        for plane in planes:
            plane.step(s)
            drip.some(EARLY_STEPS)
        if s == 1:
            for j in range(at.nfm):
                along.forward((at.f + at.nfm - j) % at.nfm)
    for s in range(at.nf):
        if tabs:
            tabs.sides(s)
        for plane in planes:
            plane.sides(s)
            drip.some(EARLY_SIDES)
        if s == 0:
            if residues:
                residues.finish()
        else:
            turns.some(1)
    drip.some(len(drip.left))
    turns.some(early_count)
    turns.some(1)
    if tabs:
        for f in range(at.nfm):
            beside.forward((at.f + f) % at.nfm)
        beside.landed()
        beside.finish()
        tabs.finish()
    along.landed()
    along.finish()
    for plane in planes:
        plane.finish()
    local.wait()
    turns.finish()
    for j in range(1, at.nfm):
        remote(mine, mine, as_sem.at[j - 1], ar_sem.at[j - 1], at.fm_device(at.f)).wait_send()


def share_inputs(sizes, tokens_in, old_weights, old_first, old_second, tables, early_count=0):
    n_dp, nf, nm = sizes
    nfm = nf * nm
    rows, columns = old_weights.shape[1:]
    dma = pltpu.SemaphoreType.DMA
    return pl.pallas_call(
        functools.partial(inputs_kernel, sizes, early_count),
        out_shape=(
            jax.ShapeDtypeStruct((nfm,) + tokens_in.shape, tokens_in.dtype),
            jax.ShapeDtypeStruct((n_dp * nfm, 3, rows, columns // nfm), old_weights.dtype),
        )
        + ((jax.ShapeDtypeStruct((early_count, n_dp * nfm, rows // n_dp, columns // nfm), old_first.dtype),) if early_count else ())
        + ((jax.ShapeDtypeStruct((n_dp * nfm,) + tables.shape, tables.dtype),) if early_count else ()),
        in_specs=[ANY, ANY, ANY, ANY, ANY],
        out_specs=(ANY, ANY, ANY, ANY) if early_count else (ANY, ANY),
        scratch_shapes=[dma((nfm - 1,)), dma((nfm - 1,)), dma((1,))]
        + PlaneSpread.sems(sizes) * IN_CHUNKS
        + DpSpread.sems(sizes)
        + (PlaneSpread.sems(sizes) + DpSpread.sems(sizes) if early_count else [])
        + (Residues.scratch(sizes) + moment_scratch(sizes, early_count, rows, columns) if early_count else []),
        compiler_params=pltpu.CompilerParams(collective_id=0, has_side_effects=True),
        name="share_inputs",
    )(tokens_in, old_weights, old_first, old_second, tables)


def outputs_kernel(sizes, att_ref, w_ref, aall_ref, oall_ref, *sems):
    at = Where(sizes)
    plane = PlaneSpread(at, att_ref, aall_ref, sems[:6])
    along = DpSpread(at, oall_ref, sems[12:16])
    wide = PlaneSpread(at, w_ref.at[3], oall_ref, sems[6:12], at.d * at.nfm, along.send)
    at.greet()
    plane.begin()
    wide.begin()
    for s in range(1, at.nf):
        plane.step(s)
        wide.step(s)
    for s in range(at.nf):
        plane.sides(s)
        wide.sides(s)
    for f in range(at.nfm):
        along.forward((at.f + f) % at.nfm)
    along.landed()
    along.finish()
    plane.finish()
    wide.finish()


def share_outputs(sizes, attended, old_weights):
    n_dp, nf, nm = sizes
    nfm = nf * nm
    rows, columns = old_weights.shape[1:]
    return pl.pallas_call(
        functools.partial(outputs_kernel, sizes),
        out_shape=(
            jax.ShapeDtypeStruct((nfm,) + attended.shape, attended.dtype),
            jax.ShapeDtypeStruct((n_dp * nfm, rows, columns), old_weights.dtype),
        ),
        in_specs=[ANY, ANY],
        out_specs=(ANY, ANY),
        scratch_shapes=PlaneSpread.sems(sizes) + PlaneSpread.sems(sizes) + DpSpread.sems(sizes),
        compiler_params=pltpu.CompilerParams(collective_id=1, has_side_effects=True),
        name="share_outputs",
    )(attended, old_weights)


def keep_residue(full, wide_ref, chosen_ref, res, dp_count):
    rows = wide_ref.shape[1] // dp_count
    for c in range(wide_ref.shape[0]):
        at = slice(c * LANES, (c + 1) * LANES)
        wide_ref[c] = full[:, at].astype(jnp.float32)
        chosen_ref[:, at] = wide_ref[c, pl.ds(res, rows, stride=dp_count), :].astype(chosen_ref.dtype)


def attend_kernel(
    dp_count, place_ref, res_ref, x_ref, wall_ref, segr_ref, segc_ref, att_ref, kept_ref, wbuf, wide, q_ref, k_ref, v_ref, sems
):
    blocks, _, rows, _ = wall_ref.shape
    seq, group = att_ref.shape

    def fetch(p):
        at = pl.ds(pl.multiple_of(place_ref[p] * rows, rows), rows)
        return pltpu.make_async_copy(wall_ref.at[p], wbuf.at[:, at], sems.at[p])

    for p in range(blocks):
        fetch(p).start()
    for p in range(blocks):
        fetch(p).wait()
    tile = 256

    def project(i, carry):
        at = pl.ds(pl.multiple_of(i * tile, tile), tile)
        x = x_ref[at, :]
        for m, ref in enumerate((q_ref, k_ref, v_ref)):
            ref[at, :] = jnp.dot(x, wbuf[m], preferred_element_type=jnp.float32).astype(jnp.bfloat16)
        return carry

    lax.fori_loop(0, seq // tile, project, 0)
    scale = 1.0 / math.sqrt(HD)
    for i in range(seq // tile):
        low, high = i * tile, (i + 1) * tile
        rowid = lax.broadcasted_iota(jnp.int32, (tile, high), 0) + low
        colid = lax.broadcasted_iota(jnp.int32, (tile, high), 1)
        allowed = (rowid >= colid) & (segc_ref[low:high, :1] == segr_ref[:1, :high])
        for h in range(group // HD):
            cols = slice(h * HD, (h + 1) * HD)
            scores = lax.dot_general(
                q_ref[low:high, cols], k_ref[:high, cols], (((1,), (1,)), ((), ())), preferred_element_type=jnp.float32
            )
            scores = jnp.where(allowed, scores * scale, -1e30)
            expo = jnp.exp(scores - jnp.max(scores, axis=1, keepdims=True))
            soft = (expo / jnp.sum(expo, axis=1, keepdims=True)).astype(jnp.bfloat16)
            out = jnp.dot(soft, v_ref[:high, cols], preferred_element_type=jnp.float32)
            att_ref[low:high, cols] = out.astype(jnp.bfloat16)
    for m in range(3):
        keep_residue(wbuf.at[m], wide, kept_ref.at[m], res_ref[0], dp_count)


def attend(dp_count, place, own_res, x_full, wall, segments):
    seq, width = x_full.shape
    blocks, _, rows, group = wall.shape
    bf16, f32 = jnp.bfloat16, jnp.float32
    return pl.pallas_call(
        functools.partial(attend_kernel, dp_count),
        out_shape=(
            jax.ShapeDtypeStruct((seq, group), bf16),
            jax.ShapeDtypeStruct((3, width // dp_count, group), bf16),
        ),
        in_specs=[SMEM, SMEM, VMEM, ANY, VMEM, VMEM],
        out_specs=(VMEM, VMEM),
        scratch_shapes=[
            pltpu.VMEM((3, width, group), bf16),
            pltpu.VMEM((group // LANES, width, LANES), f32),
            pltpu.VMEM((seq, group), bf16),
            pltpu.VMEM((seq, group), bf16),
            pltpu.VMEM((seq, group), bf16),
            pltpu.SemaphoreType.DMA((blocks,)),
        ],
        compiler_params=pltpu.CompilerParams(vmem_limit_bytes=VMEM_MOST),
        cost_estimate=pl.CostEstimate(flops=8 * 10**9, bytes_accessed=3 * 10**7, transcendentals=10**6),
        name="attend",
    )(place, own_res, x_full, wall, segments[None, :], segments[:, None])


class Scalars:
    def __init__(self, table, lane):
        self.table, self.lane = table, lane

    def __getitem__(self, p):
        return self.table[p, self.lane]


def attend_close_kernel(
    dp_count, fm_count, x_ref, wall_ref, tab_ref, att_ref, kept_ref, cols_ref, holder_ref, all_res_ref, block_ref,
    wbuf, wide, q_ref, k_ref, v_ref, sems, blocks_v, rows_s, segr, own_res, tsems,
):
    devices = tab_ref.shape[0]
    d = lax.axis_index("dp")
    vectors = pltpu.make_async_copy(tab_ref, blocks_v, tsems.at[0])
    scalars = pltpu.make_async_copy(tab_ref.at[:, 2], rows_s, tsems.at[1])
    vectors.start()
    scalars.start()
    vectors.wait()
    scalars.wait()
    for f in range(fm_count):
        block = blocks_v[d * fm_count + f]
        here = slice(f * LANES, (f + 1) * LANES)
        segr[:, here] = block[:1]
        cols_ref[here, :] = block.T
    for p in range(devices):
        block_ref[p] = rows_s[p, 0]
        holder_ref[rows_s[p, 0]] = p
    for i in range(dp_count):
        all_res_ref[i] = rows_s[i * fm_count, 1]
    own_res[0] = rows_s[d * fm_count, 1]
    attend_kernel(
        dp_count, Scalars(rows_s, 0), own_res, x_ref, wall_ref, segr, cols_ref, att_ref, kept_ref, wbuf, wide,
        q_ref, k_ref, v_ref, sems,
    )


def attend_close(sizes, x_full, wall, tables):
    dp_count, fm_count = sizes[0], sizes[1] * sizes[2]
    seq, width = x_full.shape
    devices, _, rows, group = wall.shape
    bf16, f32, i32 = jnp.bfloat16, jnp.float32, jnp.int32
    return pl.pallas_call(
        functools.partial(attend_close_kernel, dp_count, fm_count),
        out_shape=(
            jax.ShapeDtypeStruct((seq, group), bf16),
            jax.ShapeDtypeStruct((3, width // dp_count, group), bf16),
            jax.ShapeDtypeStruct((seq, 8), i32),
            jax.ShapeDtypeStruct((devices,), i32),
            jax.ShapeDtypeStruct((dp_count,), i32),
            jax.ShapeDtypeStruct((devices,), i32),
        ),
        in_specs=[VMEM, ANY, ANY],
        out_specs=(VMEM, VMEM, VMEM, SMEM, SMEM, SMEM),
        scratch_shapes=[
            pltpu.VMEM((3, width, group), bf16),
            pltpu.VMEM((group // LANES, width, LANES), f32),
            pltpu.VMEM((seq, group), bf16),
            pltpu.VMEM((seq, group), bf16),
            pltpu.VMEM((seq, group), bf16),
            pltpu.SemaphoreType.DMA((devices,)),
            pltpu.VMEM(tables.shape, i32),
            pltpu.SMEM((devices, LANES), i32),
            pltpu.VMEM((1, seq), i32),
            pltpu.SMEM((1,), i32),
            pltpu.SemaphoreType.DMA((2,)),
        ],
        compiler_params=pltpu.CompilerParams(vmem_limit_bytes=VMEM_MOST),
        cost_estimate=pl.CostEstimate(flops=8 * 10**9, bytes_accessed=3 * 10**7, transcendentals=10**6),
        name="attend",
    )(x_full, wall, tables)


def head_kernel(
    dp_count, place_ref, res_ref, f_ref, x_ref, a_ref, oall_ref, hw_ref, gain_ref, tgt_ref, out_ref, kept_ref,
    obuf, hbuf, wide, abuf, hid, norm, sems, hsem,
):
    blocks, rows, columns = oall_ref.shape
    tile, width = x_ref.shape
    fm_count, _, group = a_ref.shape
    vocab = hw_ref.shape[1]
    chunk = 256

    def fetch(p):
        at = pl.ds(pl.multiple_of(place_ref[p] * rows, rows), rows)
        return pltpu.make_async_copy(oall_ref.at[p], obuf.at[at], sems.at[p])

    def fetch_head():
        return pltpu.make_async_copy(hw_ref, hbuf, hsem.at[0])

    @pl.when(pl.program_id(0) == 0)
    def _():
        for p in range(blocks):
            fetch(p).start()
        fetch_head().start()
        for p in range(blocks):
            fetch(p).wait()

    for f in range(fm_count):
        abuf[:, f * group : (f + 1) * group] = a_ref[f]

    def hidden(i, total):
        at = pl.ds(pl.multiple_of(i * chunk, chunk), chunk)
        part = lax.dot_general(
            abuf[...], obuf[at, :], (((1,), (1,)), ((), ())), preferred_element_type=jnp.float32
        )
        part = part + x_ref[:, at].astype(jnp.float32)
        hid[:, at] = part
        return total + jnp.sum(part * part, axis=1, keepdims=True)

    total = lax.fori_loop(0, width // chunk, hidden, jnp.zeros((tile, 1), jnp.float32))
    scale = lax.rsqrt(total / width + 1e-05)

    def normed(i, carry):
        at = pl.ds(pl.multiple_of(i * chunk, chunk), chunk)
        norm[:, at] = (hid[:, at] * scale * gain_ref[:, at]).astype(jnp.bfloat16)
        return carry

    lax.fori_loop(0, width // chunk, normed, 0)

    @pl.when(pl.program_id(0) == 0)
    def _():
        fetch_head().wait()
        own = pl.ds(pl.multiple_of(f_ref[0] * group, group), group)
        keep_residue(obuf[:, own], wide, kept_ref, res_ref[0], dp_count)

    local = tgt_ref[:, :1] - f_ref[0] * vocab
    lane = lax.broadcasted_iota(jnp.int32, (tile, chunk), 1)

    def score(i, carry):
        top, total, picked = carry
        at = pl.ds(pl.multiple_of(i * chunk, chunk), chunk)
        logits = jnp.dot(norm[...], hbuf[:, at], preferred_element_type=jnp.float32)
        higher = jnp.maximum(top, jnp.max(logits, axis=1, keepdims=True))
        total = total * jnp.exp(top - higher) + jnp.sum(jnp.exp(logits - higher), axis=1, keepdims=True)
        hit = jnp.where(lane + i * chunk == local, logits, 0.0)
        return higher, total, picked + jnp.sum(hit, axis=1, keepdims=True)

    zero = jnp.zeros((tile, 1), jnp.float32)
    top, total, picked = lax.fori_loop(0, vocab // chunk, score, (zero - 1e30, zero, zero))
    lanes = lax.broadcasted_iota(jnp.int32, (tile, 128), 1)
    out_ref[...] = jnp.where(lanes == 0, top, jnp.where(lanes == 1, total, picked))


def head_parts(dp_count, place, own_res, own_f, x_full, a_all, oall, head_weight, norm_gain, targets):
    seq, width = x_full.shape
    fm_count, _, group = a_all.shape
    blocks, rows, columns = oall.shape
    vocab = head_weight.shape[1]
    tile = 256
    bf16, f32 = jnp.bfloat16, jnp.float32
    return pl.pallas_call(
        functools.partial(head_kernel, dp_count),
        grid=(seq // tile,),
        out_shape=(
            jax.ShapeDtypeStruct((seq, 128), f32),
            jax.ShapeDtypeStruct((width // dp_count, group), bf16),
        ),
        in_specs=[
            SMEM,
            SMEM,
            SMEM,
            pl.BlockSpec((tile, width), lambda i: (i, 0)),
            pl.BlockSpec((fm_count, tile, group), lambda i: (0, i, 0)),
            ANY,
            ANY,
            pl.BlockSpec((1, width), lambda i: (0, 0)),
            pl.BlockSpec((tile, 1), lambda i: (i, 0)),
        ],
        out_specs=(
            pl.BlockSpec((tile, 128), lambda i: (i, 0)),
            pl.BlockSpec((width // dp_count, group), lambda i: (0, 0)),
        ),
        scratch_shapes=[
            pltpu.VMEM((width, columns), bf16),
            pltpu.VMEM((width, vocab), bf16),
            pltpu.VMEM((group // LANES, width, LANES), f32),
            pltpu.VMEM((tile, columns), bf16),
            pltpu.VMEM((tile, width), f32),
            pltpu.VMEM((tile, width), bf16),
            pltpu.SemaphoreType.DMA((blocks,)),
            pltpu.SemaphoreType.DMA((1,)),
        ],
        compiler_params=pltpu.CompilerParams(vmem_limit_bytes=VMEM_MOST),
        cost_estimate=pl.CostEstimate(flops=2 * 10**10, bytes_accessed=4 * 10**7, transcendentals=10**6),
        name="head_parts",
    )(place, own_res, own_f, x_full, a_all, oall, head_weight, norm_gain[None, :], targets[:, None])


def in_blocks(wall, table, holder):
    if wall.shape[-2] % 16 == 0:
        return wall, table
    ordered = jnp.take(wall, holder, axis=0, mode="clip")
    blocks, rows = ordered.shape[0], ordered.shape[-2]
    join = 16 // math.gcd(16, rows)
    middle = ordered.shape[1:-2]
    ordered = ordered.reshape((blocks // join, join) + middle + ordered.shape[-2:])
    ordered = jnp.moveaxis(ordered, 1, -3)
    ordered = ordered.reshape((blocks // join,) + middle + (join * rows, ordered.shape[-1]))
    return ordered, jnp.arange(blocks // join, dtype=jnp.int32)


def body(
    sizes,
    tokens_in,
    segment_ids,
    target_ids,
    old_weights,
    old_first,
    old_second,
    old_block,
    new_residue,
    norm_gain,
    head_weight,
):
    dp_count, nf, nm = sizes
    fm_count = nf * nm
    segments, targets, table, residues = share_tables(segment_ids, target_ids, old_block, new_residue)
    holder = inverse_of(table)
    own_f = lax.axis_index(("fsdp", "mp"))[None]
    first_sent = pack_moments(old_first, residues, fm_count)
    second_sent = pack_moments(old_second, residues, fm_count)
    first_got = lax.all_to_all(first_sent, EVERYONE, split_axis=0, concat_axis=0, tiled=True)
    second_got = lax.all_to_all(second_sent, EVERYONE, split_axis=0, concat_axis=0, tiled=True)
    x_all, wall = share_inputs(sizes, tokens_in, old_weights, old_first, old_second, table)
    x_full = x_all.reshape(-1, tokens_in.shape[1])
    wall, place = in_blocks(wall, table, holder)
    attended, kept = attend(dp_count, place, new_residue, x_full, wall, segments)
    a_all, oall = share_outputs(sizes, attended, old_weights)
    oall, place = in_blocks(oall, table, holder)
    parts, kept_out = head_parts(
        dp_count, place, new_residue, own_f, x_full, a_all, oall, head_weight, norm_gain, targets
    )
    loss = joint_loss(parts[:, :3].T)
    new_weights = jnp.concatenate([kept, kept_out[None]])
    new_first = unpack_moments(first_got, table, holder)
    new_second = unpack_moments(second_got, table, holder)
    return (new_weights, new_first, new_second, loss)


def final_kernel(
    sizes, early_count, holder_ref, res_ref, att_ref, w_ref, first_ref, second_ref, x_ref, hw_ref, gain_ref,
    tgt_ref, out_ref, kept_ref, got_ref, owall, obuf, xbuf, hbuf, abuf, hid, norm, wide, wsem, *sems,
):
    at = Where(sizes)
    blocks, rows, columns = owall.shape
    seq, width = xbuf.shape
    _, _, group = abuf.shape
    vocab = hbuf.shape[1]
    tiles = seq // ROW_TILE
    chunk = 256
    pieces = got_ref.shape[0]
    step = len(PlaneSpread.sems(sizes))
    planes, sems = plane_chunks(at, att_ref, abuf, sems, ROW_TILE)
    along = DpSpread(at, owall, sems[step : step + 4])
    whole = PlaneSpread(at, w_ref.at[3], owall, sems[:step], at.d * at.nfm, along.send)
    sems = sems[step + 4 :]
    land, sent, sems = sems[:pieces], sems[pieces], sems[pieces + 1 :]
    moments = Moments(at, (first_ref, second_ref), early_count, res_ref, land, sent, got_ref, sems)
    loads = [pltpu.make_async_copy(x_ref, xbuf, wsem.at[0]), pltpu.make_async_copy(hw_ref, hbuf, wsem.at[1])]
    at.greet(diagonal=True)
    whole.begin()
    for plane in planes:
        plane.begin()
    for load in loads:
        load.start()
    drip = Drip(moments.start, range(pieces), at.nfm)
    turns = Turns(moments, drip, pieces)
    for s in range(1, at.nf):
        for plane in [whole] + planes:
            plane.step(s)
            drip.some(LATE_STEPS)
    for s in range(at.nf):
        for plane in [whole] + planes:
            plane.sides(s)
            drip.some(LATE_SIDES)
        if s >= TURN_FROM:
            turns.some(1)
    drip.some(len(drip.left))
    turns.some(TURNS)
    for f in range(at.nfm):
        along.forward((at.f + f) % at.nfm)
    turns.some(TURNS_AFTER)
    along.landed()
    own = whole.slot(at.z, at.y)
    pltpu.make_async_copy(whole.own, own, whole.lc.at[0]).wait()

    def order(b, carry):
        obuf[pl.ds(pl.multiple_of(b * rows, rows), rows), :] = owall[holder_ref[b]]
        return carry

    lax.fori_loop(0, blocks, order, 0)
    for load in loads:
        load.wait()
    for plane in planes:
        pltpu.make_async_copy(plane.own, plane.slot(at.z, at.y), plane.lc.at[0]).wait()
    lane = lax.broadcasted_iota(jnp.int32, (ROW_TILE, chunk), 1)
    lanes = lax.broadcasted_iota(jnp.int32, (ROW_TILE, LANES), 1)

    def one_tile(t, carry):
        here = pl.ds(pl.multiple_of(t * ROW_TILE, ROW_TILE), ROW_TILE)

        def hidden(i, total):
            cols = pl.ds(pl.multiple_of(i * chunk, chunk), chunk)
            part = xbuf[here, cols].astype(jnp.float32)
            for f in range(at.nfm):
                part += lax.dot_general(
                    abuf[f, here, :],
                    obuf[cols, f * group : (f + 1) * group],
                    (((1,), (1,)), ((), ())),
                    preferred_element_type=jnp.float32,
                )
            hid[:, cols] = part
            return total + jnp.sum(part * part, axis=1, keepdims=True)

        total = lax.fori_loop(0, width // chunk, hidden, jnp.zeros((ROW_TILE, 1), jnp.float32))
        scale = lax.rsqrt(total / width + 1e-05)

        def normed(i, carry):
            cols = pl.ds(pl.multiple_of(i * chunk, chunk), chunk)
            norm[:, cols] = (hid[:, cols] * scale * gain_ref[:, cols]).astype(jnp.bfloat16)
            return carry

        lax.fori_loop(0, width // chunk, normed, 0)
        local = tgt_ref[here, 1:2] - at.f * vocab

        def score(i, carry):
            top, total, picked = carry
            cols = pl.ds(pl.multiple_of(i * chunk, chunk), chunk)
            logits = jnp.dot(norm[...], hbuf[:, cols], preferred_element_type=jnp.float32)
            higher = jnp.maximum(top, jnp.max(logits, axis=1, keepdims=True))
            total = total * jnp.exp(top - higher) + jnp.sum(jnp.exp(logits - higher), axis=1, keepdims=True)
            hit = jnp.where(lane + i * chunk == local, logits, 0.0)
            return higher, total, picked + jnp.sum(hit, axis=1, keepdims=True)

        zero = jnp.zeros((ROW_TILE, 1), jnp.float32)
        top, total, picked = lax.fori_loop(0, vocab // chunk, score, (zero - 1e30, zero, zero))
        out_ref[here, :] = jnp.where(lanes == 0, top, jnp.where(lanes == 1, total, picked))
        return carry

    for t in range(tiles):
        lax.fori_loop(t, t + 1, one_tile, 0)
        turns.some(1)
    part_rows = wide.shape[0]
    for c in range(group // LANES):
        cols = pl.ds(pl.multiple_of(at.f * group + c * LANES, LANES), LANES)
        for i in range(width // part_rows):
            wide[...] = obuf[i * part_rows : (i + 1) * part_rows, cols].astype(jnp.float32)
            kept = wide[pl.ds(res_ref[at.d], part_rows // at.n_dp, stride=at.n_dp), :]
            kept_rows = part_rows // at.n_dp
            kept_ref[i * kept_rows : (i + 1) * kept_rows, c * LANES : (c + 1) * LANES] = kept.astype(kept_ref.dtype)
    turns.some(pieces)
    turns.some(1)
    along.finish()
    for plane in planes + [whole]:
        plane.sent()
    turns.finish()


def finish_all(sizes, early_count, holder, residues, attended, old_weights, old_first, old_second, x_full,
               head_weight, norm_gain, columns_in):
    n_dp, nf, nm = sizes
    nfm = nf * nm
    matrices, rows, columns = old_weights.shape
    seq, width = x_full.shape
    vocab = head_weight.shape[1]
    group, devices, pair_rows = columns // nfm, n_dp * nfm, rows // n_dp
    pieces = 2 * matrices - early_count
    bf16, f32 = jnp.bfloat16, jnp.float32
    plane_sems = PlaneSpread.sems(sizes)
    return pl.pallas_call(
        functools.partial(final_kernel, sizes, early_count),
        out_shape=(
            jax.ShapeDtypeStruct((seq, LANES), f32),
            jax.ShapeDtypeStruct((width // n_dp, group), bf16),
            jax.ShapeDtypeStruct((pieces, devices, pair_rows, group), f32),
        ),
        in_specs=[SMEM, SMEM] + [ANY] * 6 + [VMEM, VMEM],
        out_specs=(VMEM, VMEM, ANY),
        scratch_shapes=[
            pltpu.VMEM((devices, rows, columns), bf16),
            pltpu.VMEM((width, columns), bf16),
            pltpu.VMEM((seq, width), bf16),
            pltpu.VMEM((width, vocab), bf16),
            pltpu.VMEM((nfm, seq, group), bf16),
            pltpu.VMEM((ROW_TILE, width), f32),
            pltpu.VMEM((ROW_TILE, width), bf16),
            pltpu.VMEM((width // 4, LANES), f32),
            pltpu.SemaphoreType.DMA((2,)),
        ]
        + plane_sems * (seq // ROW_TILE + 1)
        + DpSpread.sems(sizes)
        + moment_scratch(sizes, pieces, rows, columns),
        compiler_params=pltpu.CompilerParams(
            collective_id=2, has_side_effects=True, vmem_limit_bytes=63 * 1024 * 1024
        ),
        cost_estimate=pl.CostEstimate(flops=2 * 10**10, bytes_accessed=4 * 10**7, transcendentals=10**6),
        name="finish_all",
    )(holder, residues, attended, old_weights, old_first, old_second, x_full, head_weight, norm_gain[None, :],
      columns_in)


def body_close(
    sizes,
    tokens_in,
    segment_ids,
    target_ids,
    old_weights,
    old_first,
    old_second,
    old_block,
    new_residue,
    norm_gain,
    head_weight,
):
    scalars = jnp.pad(jnp.concatenate([old_block, new_residue]), (0, LANES - 2))
    own = jnp.pad(jnp.stack([segment_ids, target_ids, scalars]), ((0, 5), (0, 0)))
    x_all, wall, got_early, tables = share_inputs(sizes, tokens_in, old_weights, old_first, old_second, own, EARLY)
    x_full = x_all.reshape(-1, tokens_in.shape[1])
    attended, kept, columns, holder, residues, table = attend_close(sizes, x_full, wall, tables)
    parts, kept_out, got = finish_all(
        sizes, EARLY, holder, residues, attended, old_weights, old_first, old_second, x_full, head_weight,
        norm_gain, columns,
    )
    loss = joint_loss(parts[:, :3].T)
    new_weights, new_first, new_second = unpack_all(table, got_early, got, kept, kept_out)
    return (new_weights, new_first, new_second, loss)


def solution(mesh):
    placed = (
        P(EVERYONE, None),
        P(EVERYONE),
        P(EVERYONE),
        P(None, EVERYONE, None),
        P(None, EVERYONE, None),
        P(None, EVERYONE, None),
        P(EVERYONE),
        P("dp"),
        P(),
        P(None, ("fsdp", "mp")),
    )
    sizes = tuple(mesh.shape[name] for name in EVERYONE)

    def step(*args):
        rows, columns = args[3].shape[1:]
        seq = args[0].shape[0] * sizes[1] * sizes[2]
        close = rows % 16 == 0 and (rows // sizes[0]) % 8 == 0 and seq <= 1024 and columns <= 2048
        close = close and args[1].shape[0] == LANES
        return (body_close if close else body)(sizes, *args)

    return jax.shard_map(
        step,
        mesh=mesh,
        in_specs=placed,
        out_specs=(
            P(None, "dp", ("fsdp", "mp")),
            P(None, "dp", ("fsdp", "mp")),
            P(None, "dp", ("fsdp", "mp")),
            P(EVERYONE),
        ),
        check_vma=False,
    )
```
